512 devices in a mesh: grp: 32 (over z_lo, y, core), fsdp: 16 (over x, z_hi).
Axes of the slice: x: 4, y: 4, z: 16 (z_hi: 4, z_lo: 4; z = z_hi * 4 + z_lo), core: 2. Of those that a mesh axis runs over, the one named last changes fastest.
Arguments:
- layer_inputs: bfloat16 [32, 8192, 2048], P('grp', 'fsdp'), may hold values from -6 to 6
- key_cotangent: bfloat16 [32, 8192, 768], P('grp', 'fsdp'), may hold values from -0.099609375 to 0.099609375
- key_weights: bfloat16 [2048, 768], P('fsdp'), may hold values from -0.125 to 0.125
- outer_momentum: float32 [2048, 768], P('fsdp'), may hold values from -0.02 to 0.02
- state_codes: int32 [32, 2048, 768], P('grp', 'fsdp'), may hold values from 0 to 255
- first_row_max: float32 [32, 2048], P('grp', 'fsdp'), may hold values from 0.1 to 2
- first_col_max: float32 [32, 768], P('grp'), may hold values from 0.1 to 2
- second_row_max: float32 [32, 2048], P('grp', 'fsdp'), may hold values from 0.1 to 4
- second_col_max: float32 [32, 768], P('grp'), may hold values from 0.1 to 4
Outputs:
- new_weights: float32 [2048, 768], P('fsdp')
- new_momentum: float32 [2048, 768], P('fsdp')
- first_state: bfloat16 [32, 2048, 768], P('grp', 'fsdp')
- second_state: bfloat16 [32, 2048, 768], P('grp', 'fsdp')
- new_first_row_max: float32 [32, 2048], P('grp', 'fsdp')
- new_first_col_max: float32 [32, 768], P('grp')
- new_second_row_max: float32 [32, 2048], P('grp', 'fsdp')
- new_second_col_max: float32 [32, 768], P('grp')
- next_keys: bfloat16 [32, 8192, 768], P('grp', 'fsdp')
The draws below stay inside these ranges and needn't reach their ends.
All inputs are finite; a program needn't handle non-finite values. Where the reference program divides by a largest or mean magnitude, that divisor is 1e-20 or more.
Results may differ from the reference program's by a relative error of at most 0.018.
Values may be sent and summed in bfloat16 or wider, within the bound.
A program may use at most 64 MiB of HBM per device.

```python
import math
import jax
import jax.numpy as jnp
from jax import lax

ROWS = 2048
COLS = 768
TOK_DEV = 512
GROUPS = 32
TOK_GRP = 8192
N_GRP = 32
N_FSDP = 16


def set_ends(result, own_key, low, top_value):
    place = [jax.random.randint(jax.random.fold_in(own_key, axis), (), 0, length) for axis, length in enumerate(result.shape)]
    main_axis = result.shape.index(max(result.shape))
    beside = place[:main_axis] + [(place[main_axis] + 1) % result.shape[main_axis]] + place[main_axis + 1:]
    return result.at[tuple(place)].set(low).at[tuple(beside)].set(top_value)


def shard_levels(own_key, shape, shards, smallest, high):
    level = 1.0
    for position, shards_of in shards:
        steps = jax.random.uniform(jax.random.fold_in(jax.random.fold_in(own_key, 6), position), (shards_of,), jnp.float32, smallest / len(shards), high / len(shards))
        level = level * jnp.repeat(jnp.exp(steps), shape[position] // shards_of).reshape((-1,) + (1,) * (len(shape) - 1 - position))
    return level


def bell_draw(stream_key, shape, width, bound, cuts=(), dtype=jnp.bfloat16):
    entries = jax.random.normal(stream_key, shape, jnp.float32) * width
    if len(cuts) > 0:
        entries = shard_levels(stream_key, shape, cuts, -0.22, 0.18) * entries
    return jnp.clip(entries, min=-bound, max=bound).astype(dtype)


def setup_inputs(seed: int = 0) -> dict:
    streams_of = jax.random.split(jax.random.key(seed), 10)
    layer_inputs = bell_draw(streams_of[0], (GROUPS, TOK_GRP, ROWS), 1.0, 6.0, ((0, 32), (1, 16)))
    key_cotangent = bell_draw(streams_of[1], (GROUPS, TOK_GRP, COLS), 0.015625, 0.099609375, ((0, 32), (1, 16)))
    key_weights = bell_draw(streams_of[2], (ROWS, COLS), ROWS ** -0.5, 0.125, ((0, 16),))
    outer_momentum = bell_draw(streams_of[3], (ROWS, COLS), 0.003, 0.02, ((0, 16),), jnp.float32)
    state_codes = set_ends(jax.random.randint(streams_of[4], (GROUPS, ROWS, COLS), 0, 256), jax.random.fold_in(streams_of[4], 1), 0, 255).astype(jnp.int32)
    first_row_max = jnp.clip(jnp.exp(math.log(2.0) - 2.9957323 * jax.random.uniform(streams_of[5], (GROUPS, ROWS), jnp.float32) ** shard_levels(streams_of[5], (GROUPS, ROWS), ((0, 32), (1, 16)), -0.2, 0.2)), 0.1, 2.0)
    first_col_max = jnp.clip(jnp.exp(math.log(2.0) - 2.9957323 * jax.random.uniform(streams_of[6], (GROUPS, COLS), jnp.float32) ** shard_levels(streams_of[6], (GROUPS, COLS), ((0, 32),), -0.2, 0.2)), 0.1, 2.0)
    second_row_max = jnp.clip(jnp.exp(math.log(4.0) - 3.6888794 * jax.random.uniform(streams_of[7], (GROUPS, ROWS), jnp.float32) ** shard_levels(streams_of[7], (GROUPS, ROWS), ((0, 32), (1, 16)), -0.2, 0.2)), 0.1, 4.0)
    second_col_max = jnp.clip(jnp.exp(math.log(4.0) - 3.6888794 * jax.random.uniform(streams_of[8], (GROUPS, COLS), jnp.float32) ** shard_levels(streams_of[8], (GROUPS, COLS), ((0, 32),), -0.2, 0.2)), 0.1, 4.0)
    return dict(layer_inputs=layer_inputs, key_cotangent=key_cotangent, key_weights=key_weights, outer_momentum=outer_momentum, state_codes=state_codes, first_row_max=first_row_max, first_col_max=first_col_max, second_row_max=second_row_max, second_col_max=second_col_max)


beta_one = 0.9
beta_two = 0.95
bias_one = 1.0 - 0.9 ** 10
bias_two = 1.0 - 0.95 ** 10
adam_eps = 1e-08
inner_rate = 0.01
weight_decay = 0.1
outer_rate = 0.7
outer_beta = 0.9
stat_eps = 1e-06

def adam_moments(gradient, packed_codes, first_rows, first_cols, second_rows, second_cols):
    first_code = (packed_codes // 16).astype(jnp.float32)
    second_code = (packed_codes % 16).astype(jnp.float32)
    first_old = jnp.minimum(first_rows[:, None], first_cols[None, :]) * (first_code - 7.5) / 7.5
    second_old = jnp.minimum(second_rows[:, None], second_cols[None, :]) * ((second_code + 1.0) / 16.0) ** 2
    first_new = beta_one * first_old + (1.0 - beta_one) * gradient
    second_new = beta_two * second_old + (1.0 - beta_two) * gradient * gradient
    return (first_new, second_new)

def pseudo_step(first_new, second_new, weights_float):
    update = first_new / bias_one / (jnp.sqrt(second_new / bias_two) + adam_eps)
    return inner_rate * (update + weight_decay * weights_float)

def reference(layer_inputs, key_cotangent, key_weights, outer_momentum, state_codes, first_row_max, first_col_max, second_row_max, second_col_max):
    weights_float = key_weights.astype(jnp.float32)

    def group_step(running, inputs):
        tokens, cotangent, packed_codes, first_rows, first_cols, second_rows, second_cols = inputs
        token_blocks = tokens.reshape(N_FSDP, TOK_DEV, ROWS)
        grad_blocks = cotangent.reshape(N_FSDP, TOK_DEV, COLS)

        def add_term(accum, pair):
            partial_term = lax.dot_general(pair[0], pair[1], (((0,), (0,)), ((), ())), preferred_element_type=jnp.float32)
            rounded = lax.optimization_barrier(partial_term.astype(jnp.bfloat16))
            return (accum + rounded.astype(jnp.float32), None)
        gradient, unused = lax.scan(add_term, jnp.zeros((ROWS, COLS), jnp.float32), (token_blocks, grad_blocks))
        first_new, second_new = adam_moments(gradient, packed_codes, first_rows, first_cols, second_rows, second_cols)
        pseudo = pseudo_step(first_new, second_new, weights_float)
        first_rmax = lax.optimization_barrier(jnp.max(jnp.abs(first_new), axis=1)) + stat_eps
        first_cmax = lax.optimization_barrier(jnp.max(jnp.abs(first_new), axis=0)) + stat_eps
        second_rmax = lax.optimization_barrier(jnp.max(second_new, axis=1)) + stat_eps
        second_cmax = lax.optimization_barrier(jnp.max(second_new, axis=0)) + stat_eps
        first_state = (first_new / jnp.minimum(first_rmax[:, None], first_cmax[None, :])).astype(jnp.bfloat16)
        second_state = (second_new / jnp.minimum(second_rmax[:, None], second_cmax[None, :])).astype(jnp.bfloat16)
        return (running + pseudo, (first_state, second_state, first_rmax, first_cmax, second_rmax, second_cmax))
    running, results = lax.scan(group_step, jnp.zeros((ROWS, COLS), jnp.float32), (layer_inputs, key_cotangent, state_codes, first_row_max, first_col_max, second_row_max, second_col_max))
    averaged = running / N_GRP
    new_momentum = outer_beta * outer_momentum + averaged
    new_weights = weights_float - outer_rate * (averaged + outer_beta * new_momentum)
    weights_half = new_weights.astype(jnp.bfloat16)

    def project(tokens):
        return jnp.dot(tokens, weights_half, preferred_element_type=jnp.float32).astype(jnp.bfloat16)
    next_keys = lax.map(project, layer_inputs)
    first_state, second_state, first_rmax, first_cmax, second_rmax, second_cmax = results
    return (new_weights, new_momentum, first_state, second_state, first_rmax, first_cmax, second_rmax, second_cmax, next_keys)
```

```python
import jax
import jax.numpy as jnp
from jax import lax
from jax.experimental import pallas as pl
from jax.experimental.pallas import tpu as pltpu
from jax.sharding import Mesh
from jax.sharding import PartitionSpec as P

MESH = pl.DeviceIdType.MESH
GRP = ("zl", "y", "core")
FSDP = ("x", "zh")

beta_one = 0.9
beta_two = 0.95
bias_one = 1.0 - 0.9**10
bias_two = 1.0 - 0.95**10
adam_eps = 1e-08
inner_rate = 0.01
weight_decay = 0.1
outer_rate = 0.7
outer_beta = 0.9
stat_eps = 1e-06

NC = 3
T = 128
bf16 = jnp.bfloat16
f32 = jnp.float32

XF, XD, XC, ZF, ZD, ZC = 0, 2, 4, 6, 8, 10
CE = 12
YS, LS, HS, AY, WY = 13, 16, 19, 22, 25
WX, WF, WC, AC = 28, 30, 32, 36
PER = 37
CX, CZ = NC * PER, NC * PER + 3
NSEM = NC * PER + 6


def kernel(
    tok, cot, wgt, omom, codes, frm, fcm, srm, scm,
    nw_o, nm_o, fs_o, ss_o, frm_o, fcm_o, srm_o, scm_o, keys_o,
    term, xr, cbuf, zf, zs, zr, zc, pf, pcs, pcr, ysf, ysb, yr, zlb, avgt, wbuf, acc,
    wf, rows, rmax, cmx, cmz, fnew, snew, ssem, rsem,
):
    x, zh = lax.axis_index("x"), lax.axis_index("zh")
    y, zl, c = lax.axis_index("y"), lax.axis_index("zl"), lax.axis_index("core")
    here = {"x": x, "zh": zh, "y": y, "zl": zl}

    def at(axis, offset):
        return lax.rem(here[axis] + (4 + offset), 4)

    def to(axis, offset):
        return {axis: at(axis, offset)}

    oc = 1 - c
    partner = {"core": oc}

    barrier = pltpu.get_barrier_semaphore()
    for axis in ("x", "zh", "y", "zl"):
        for o in (1, 2, 3):
            pl.semaphore_signal(barrier, inc=1, device_id=to(axis, o), device_id_type=MESH)
    pl.semaphore_signal(barrier, inc=1, device_id=partner, device_id_type=MESH)

    started = []

    def send(number, src, dst, device):
        copy = pltpu.make_async_remote_copy(
            src_ref=src, dst_ref=dst, send_sem=ssem.at[number], recv_sem=rsem.at[number],
            device_id=device, device_id_type=MESH,
        )
        copy.start()
        started.append(copy)

    def arrived(number, dst):
        pltpu.make_async_remote_copy(
            src_ref=dst, dst_ref=dst, send_sem=ssem.at[number], recv_sem=rsem.at[number],
            device_id=partner, device_id_type=MESH,
        ).wait_recv()

    def tile_columns(k, ab):
        return slice((2 * k + ab) * T, (2 * k + ab + 1) * T)

    def compute_term(k, slot, owner):
        @pl.loop(0, 4)
        def _(j):
            lhs = tok[0, :, pl.ds(pl.multiple_of(owner * 512 + j * T, T), T)]
            part = lax.dot_general(
                lhs, cot[0, :, 2 * k * T:(2 * k + 2) * T], (((0,), (0,)), ((), ())),
                preferred_element_type=f32,
            )
            at_rows = pl.ds(pl.multiple_of(j * T, T), T)
            term[k, slot, 0, at_rows, :] = part[:, :T].astype(bf16)
            term[k, slot, 1, at_rows, :] = part[:, T:].astype(bf16)

    def s0(k):
        compute_term(k, 0, at("x", 2))
        b = k * PER
        if k == 0:
            pl.semaphore_wait(barrier, 13)
        send(b + XF, term.at[k, 0, 0], xr.at[k, 0, 0], to("x", -1))
        send(b + XF + 1, term.at[k, 0, 1], xr.at[k, 0, 1], to("x", 1))

    def s1(k):
        b = k * PER
        compute_term(k, 1, at("x", 1))
        send(b + XD, term.at[k, 1, 0], xr.at[k, 1, 0], to("x", 1))
        compute_term(k, 2, at("x", -1))
        send(b + XD + 1, term.at[k, 2, 1], xr.at[k, 1, 1], to("x", -1))

    def s2(k):
        b = k * PER
        for ab, slot, way in ((0, 2, -1), (1, 1, 1)):
            arrived(b + XF + ab, xr.at[k, 0, ab])
            cbuf[k, ab] = (term[k, slot, ab].astype(f32) + xr[k, 0, ab].astype(f32)).astype(bf16)
            send(b + XC + ab, cbuf.at[k, ab], xr.at[k, 2, ab], to("x", way))

    def own_terms(k):
        compute_term(k, 3, x)

    def s3(k):
        b = k * PER
        for ab in (0, 1):
            arrived(b + XD + ab, xr.at[k, 1, ab])
        for ab in (0, 1):
            arrived(b + XC + ab, xr.at[k, 2, ab])

        def total(ab, block):
            at_rows = pl.ds(pl.multiple_of(block * T, T), T)
            value = (
                term[k, 3, ab, at_rows, :].astype(f32)
                + xr[k, 1, ab, at_rows, :].astype(f32)
                + xr[k, 2, ab, at_rows, :].astype(f32)
            )
            zf[k, ab, block] = value
            zs[k, ab, block] = value.astype(bf16)

        far, after, before = at("zh", 2), at("zh", 1), at("zh", -1)
        total(0, far)
        send(b + ZF, zs.at[k, 0, far], zr.at[k, 0, 0], to("zh", -1))
        total(1, far)
        send(b + ZF + 1, zs.at[k, 1, far], zr.at[k, 0, 1], to("zh", 1))
        total(0, after)
        send(b + ZD, zs.at[k, 0, after], zr.at[k, 1, 0], to("zh", 1))
        total(1, before)
        send(b + ZD + 1, zs.at[k, 1, before], zr.at[k, 1, 1], to("zh", -1))
        total(1, after)
        total(0, before)
        total(0, zh)
        total(1, zh)

    def s4(k):
        b = k * PER
        for ab, way in ((0, -1), (1, 1)):
            arrived(b + ZF + ab, zr.at[k, 0, ab])
            zc[k, ab] = (zf[k, ab, at("zh", way)] + zr[k, 0, ab].astype(f32)).astype(bf16)
            send(b + ZC + ab, zc.at[k, ab], zr.at[k, 2, ab], to("zh", way))

    def s5(k):
        b = k * PER
        for ab in (0, 1):
            arrived(b + ZD + ab, zr.at[k, 1, ab])
        for ab in (0, 1):
            arrived(b + ZC + ab, zr.at[k, 2, ab])
        for ab in (0, 1):
            cols = tile_columns(k, ab)
            gradient = zf[k, ab, zh] + zr[k, 1, ab].astype(f32) + zr[k, 2, ab].astype(f32)
            packed = codes[0, :, cols]
            first_code = (packed >> 4).astype(f32)
            second_code = (packed & 15).astype(f32)
            first_old = jnp.minimum(rows[0], fcm[:, cols]) * (first_code - 7.5) / 7.5
            level = (second_code + 1.0) / 16.0
            second_old = jnp.minimum(rows[1], scm[:, cols]) * (level * level)
            first_new = beta_one * first_old + (1.0 - beta_one) * gradient
            second_new = beta_two * second_old + (1.0 - beta_two) * gradient * gradient
            update = first_new / bias_one / (jnp.sqrt(second_new / bias_two) + adam_eps)
            pf[k, ab] = inner_rate * (update + weight_decay * wf[:, cols])
            fnew[:, cols] = first_new
            snew[:, cols] = second_new
            size = jnp.abs(first_new)
            cmx[x, 0:1, cols] = jnp.max(size, axis=0, keepdims=True)
            cmx[x, 1:2, cols] = jnp.max(second_new, axis=0, keepdims=True)
            if k == 0 and ab == 0:
                rmax[0] = size
                rmax[1] = second_new
            else:
                rmax[0] = jnp.maximum(rmax[0], size)
                rmax[1] = jnp.maximum(rmax[1], second_new)
        pcs[k] = pf[k, oc].astype(bf16)
        send(b + CE, pcs.at[k], pcr.at[k], partner)

    def s6(k):
        b = k * PER
        arrived(b + CE, pcr.at[k])
        both = pf[k, c] + pcr[k].astype(f32)
        ysf[k] = both
        ysb[k] = both.astype(bf16)
        for o in (1, 2, 3):
            theirs = pl.ds(pl.multiple_of(at("y", o) * 32, 32), 32)
            send(b + YS + o - 1, ysb.at[k, theirs, :], yr.at[k, o - 1], to("y", o))

    mine = pl.ds(pl.multiple_of(y * 32, 32), 32)

    def s7(k):
        b = k * PER
        for o in (1, 2, 3):
            arrived(b + YS + o - 1, yr.at[k, o - 1])
        zlb[k, zl] = (
            ysf[k, mine, :]
            + yr[k, 0].astype(f32) + yr[k, 1].astype(f32) + yr[k, 2].astype(f32)
        )
        for o in (1, 2, 3):
            send(b + LS + o - 1, zlb.at[k, zl], zlb.at[k, zl], to("zl", o))

    def s8(k):
        b = k * PER
        for o in (1, 2, 3):
            arrived(b + LS + o - 1, zlb.at[k, at("zl", -o)])
        averaged = ((zlb[k, 0] + zlb[k, 1]) + (zlb[k, 2] + zlb[k, 3])) / 32.0
        cols = pl.ds(pl.multiple_of((2 * k + c) * T, T), T)
        momentum = outer_beta * omom[mine, cols] + averaged
        weights = wf[mine, cols] - outer_rate * (averaged + outer_beta * momentum)
        wbuf[k, c, x, zh, mine, :] = weights.astype(bf16)
        for o in (2, 1, 3):
            piece = wbuf.at[k, c, x, zh, mine, :]
            send(b + HS + o - 1, piece, piece, to("zh", o))
        avgt[k, c, mine, :] = averaged
        for o in (1, 2, 3):
            piece = avgt.at[k, c, mine, :]
            send(b + AY + o - 1, piece, piece, to("y", o))

    def s9(k):
        b = k * PER
        for o in (1, 2, 3):
            arrived(b + HS + o - 1, wbuf.at[k, c, x, at("zh", -o), mine, :])
        for o in (2, 1, 3):
            piece = wbuf.at[k, c, x, :, mine, :]
            send(b + WY + o - 1, piece, piece, to("y", o))

    def s10(k):
        b = k * PER
        for o in (1, 2, 3):
            theirs = pl.ds(pl.multiple_of(at("y", -o) * 32, 32), 32)
            arrived(b + WY + o - 1, wbuf.at[k, c, x, :, theirs, :])
        block = wbuf.at[k, c, x]
        send(b + WX, block, block, to("x", 1))
        send(b + WX + 1, block, block, to("x", -1))
        send(b + WC, block, block, partner)

    def s11(k):
        b = k * PER
        before, after = at("x", -1), at("x", 1)
        arrived(b + WX, wbuf.at[k, c, before])
        part = wbuf.at[k, c, before, 0:2]
        send(b + WF, part, part, to("x", 1))
        arrived(b + WX + 1, wbuf.at[k, c, after])
        part = wbuf.at[k, c, after, 2:4]
        send(b + WF + 1, part, part, to("x", -1))
        for n, at_x in ((1, before), (2, after)):
            block = wbuf.at[k, c, at_x]
            send(b + WC + n, block, block, partner)

    def s12(k):
        b = k * PER
        far = at("x", 2)
        arrived(b + WF, wbuf.at[k, c, far, 0:2])
        arrived(b + WF + 1, wbuf.at[k, c, far, 2:4])
        block = wbuf.at[k, c, far]
        send(b + WC + 3, block, block, partner)

    def product(k, n, at_x):
        arrived(k * PER + WC + n, wbuf.at[k, oc, at_x])

        @pl.loop(0, 4)
        def _(j):
            at_rows = pl.ds(pl.multiple_of(j * T, T), T)
            lhs = tok[0, at_rows, pl.ds(pl.multiple_of(at_x * 512, 512), 512)]
            rhs = jnp.concatenate(
                [wbuf[k, 0, at_x].reshape(512, T), wbuf[k, 1, at_x].reshape(512, T)], axis=1
            )
            part = jnp.dot(lhs, rhs, preferred_element_type=f32)
            if n > 0:
                part = part + acc[k, at_rows, :]
            if n < 3:
                acc[k, at_rows, :] = part
            else:
                keys_o[0, at_rows, 2 * k * T:(2 * k + 2) * T] = part.astype(bf16)

    def near_products(k):
        product(k, 0, x)
        product(k, 1, at("x", -1))
        product(k, 2, at("x", 1))

    def s13(k):
        product(k, 3, at("x", 2))

    def t1(k):
        b = k * PER
        for o in (1, 2, 3):
            theirs = pl.ds(pl.multiple_of(at("y", -o) * 32, 32), 32)
            arrived(b + AY + o - 1, avgt.at[k, c, theirs, :])
        send(b + AC, avgt.at[k, c], avgt.at[k, c], partner)

    def t2(k):
        arrived(k * PER + AC, avgt.at[k, oc])
        for ab in (0, 1):
            cols = tile_columns(k, ab)
            averaged = avgt[k, ab]
            momentum = outer_beta * omom[:, cols] + averaged
            nm_o[:, cols] = momentum
            nw_o[:, cols] = wf[:, cols] - outer_rate * (averaged + outer_beta * momentum)

    def u0():
        for o in (1, 2, 3):
            send(CX + o - 1, cmx.at[x], cmx.at[x], to("x", o))

    def u1():
        for o in (1, 2, 3):
            arrived(CX + o - 1, cmx.at[at("x", -o)])
        cmz[zh] = jnp.maximum(jnp.maximum(cmx[0], cmx[1]), jnp.maximum(cmx[2], cmx[3]))
        for o in (1, 2, 3):
            send(CZ + o - 1, cmz.at[zh], cmz.at[zh], to("zh", o))

    def u2():
        for o in (1, 2, 3):
            arrived(CZ + o - 1, cmz.at[at("zh", -o)])
        cols_max = jnp.maximum(jnp.maximum(cmz[0], cmz[1]), jnp.maximum(cmz[2], cmz[3])) + stat_eps
        fcm_o[...] = cols_max[0:1]
        scm_o[...] = cols_max[1:2]
        for m, (new, rm_o, st_o) in enumerate(((fnew, frm_o, fs_o), (snew, srm_o, ss_o))):
            flipped = jnp.max(rmax[m].T, axis=0, keepdims=True) + stat_eps
            rm_o[...] = flipped
            rm = jnp.broadcast_to(flipped, (T, T)).T
            for t in range(2 * NC):
                cols = slice(t * T, (t + 1) * T)
                st_o[0, :, cols] = (
                    new[:, cols] / jnp.minimum(rm, cols_max[m:m + 1, cols])
                ).astype(bf16)

    s0(0)
    s1(0)
    s0(1)
    wf[...] = wgt[...].astype(f32)
    rows[0] = jnp.broadcast_to(frm[...], (T, T)).T
    rows[1] = jnp.broadcast_to(srm[...], (T, T)).T
    s2(0)
    s1(1)
    s0(2)
    s2(1)
    s1(2)
    own_terms(0)
    own_terms(1)
    own_terms(2)
    s3(0)
    s2(2)
    s4(0)
    s3(1)
    s5(0)
    s3(2)
    s6(0)
    s4(1)
    s7(0)
    s5(1)
    s4(2)
    s8(0)
    s6(1)
    s7(1)
    s5(2)
    u0()
    s6(2)
    s8(1)
    s9(0)
    s7(2)
    u1()
    s10(0)
    s8(2)
    s9(1)
    t1(0)
    s11(0)
    s10(1)
    t1(1)
    s12(0)
    near_products(0)
    s11(1)
    s9(2)
    s13(0)
    s12(1)
    near_products(1)
    s10(2)
    t1(2)
    s13(1)
    u2()
    t2(0)
    t2(1)
    t2(2)
    s11(2)
    product(2, 0, x)
    s12(2)
    product(2, 1, at("x", -1))
    product(2, 2, at("x", 1))
    s13(2)
    for copy in started:
        copy.wait_send()


def local(tok, cot, wgt, omom, codes, frm, fcm, srm, scm):
    def out(*shape, dtype=f32):
        return jax.ShapeDtypeStruct(shape, dtype)

    vmem = pl.BlockSpec(memory_space=pltpu.VMEM)
    return pl.pallas_call(
        kernel,
        out_shape=(
            out(128, 768), out(128, 768),
            out(1, 128, 768, dtype=bf16), out(1, 128, 768, dtype=bf16),
            out(1, 128), out(1, 768), out(1, 128), out(1, 768),
            out(1, 512, 768, dtype=bf16),
        ),
        in_specs=[vmem] * 9,
        out_specs=(vmem,) * 9,
        scratch_shapes=[
            pltpu.VMEM((NC, 4, 2, 512, T), bf16),
            pltpu.VMEM((NC, 3, 2, 512, T), bf16),
            pltpu.VMEM((NC, 2, 512, T), bf16),
            pltpu.VMEM((NC, 2, 4, T, T), f32),
            pltpu.VMEM((NC, 2, 4, T, T), bf16),
            pltpu.VMEM((NC, 3, 2, T, T), bf16),
            pltpu.VMEM((NC, 2, T, T), bf16),
            pltpu.VMEM((NC, 2, T, T), f32),
            pltpu.VMEM((NC, T, T), bf16),
            pltpu.VMEM((NC, T, T), bf16),
            pltpu.VMEM((NC, T, T), f32),
            pltpu.VMEM((NC, T, T), bf16),
            pltpu.VMEM((NC, 3, 32, T), bf16),
            pltpu.VMEM((NC, 4, 32, T), f32),
            pltpu.VMEM((NC, 2, T, T), f32),
            pltpu.VMEM((NC, 2, 4, 4, T, T), bf16),
            pltpu.VMEM((NC, 512, 2 * T), f32),
            pltpu.VMEM((T, 768), f32),
            pltpu.VMEM((2, T, T), f32),
            pltpu.VMEM((2, T, T), f32),
            pltpu.VMEM((4, 2, 768), f32),
            pltpu.VMEM((4, 2, 768), f32),
            pltpu.VMEM((T, 768), f32),
            pltpu.VMEM((T, 768), f32),
            pltpu.SemaphoreType.DMA((NSEM,)),
            pltpu.SemaphoreType.DMA((NSEM,)),
        ],
        compiler_params=pltpu.CompilerParams(
            collective_id=0, has_side_effects=True, vmem_limit_bytes=48 * 1024 * 1024
        ),
        name="round",
    )(tok, cot, wgt, omom, codes, frm, fcm, srm, scm)


def solution(mesh):
    finer = Mesh(mesh.devices.reshape(4, 4, 2, 4, 4), (*GRP, *FSDP))
    in_specs = (
        P(GRP, FSDP, None), P(GRP, FSDP, None), P(FSDP, None), P(FSDP, None),
        P(GRP, FSDP, None), P(GRP, FSDP), P(GRP, None), P(GRP, FSDP), P(GRP, None),
    )
    out_specs = (
        P(FSDP, None), P(FSDP, None), P(GRP, FSDP, None), P(GRP, FSDP, None),
        P(GRP, FSDP), P(GRP, None), P(GRP, FSDP), P(GRP, None), P(GRP, FSDP, None),
    )
    return jax.shard_map(local, mesh=finer, in_specs=in_specs, out_specs=out_specs, check_vma=False)
```

```python
import jax
import jax.numpy as jnp
from jax import lax
from jax.experimental import pallas as pl
from jax.experimental.pallas import tpu as pltpu
from jax.sharding import Mesh
from jax.sharding import PartitionSpec as P

MESH = pl.DeviceIdType.MESH
GRP = ("zl", "y", "core")
FSDP = ("x", "zh")

beta_one = 0.9
beta_two = 0.95
bias_one = 1.0 - 0.9**10
bias_two = 1.0 - 0.95**10
adam_eps = 1e-08
inner_rate = 0.01
weight_decay = 0.1
outer_rate = 0.7
outer_beta = 0.9
stat_eps = 1e-06

NC = 6
T = 128
H = 64
Q = 16
bf16 = jnp.bfloat16
f32 = jnp.float32

XF, XD, XC, ZF, ZD, ZC = 0, 2, 4, 6, 8, 10
CE = 12
YS, LS, HS, AY, WY = 13, 16, 19, 22, 25
WX, WF, WC, AC = 28, 30, 32, 36
PER = 37
CX, CZ = NC * PER, NC * PER + 3
NSEM = NC * PER + 6

SCHEDULE = (
    "ta:0", "s0:0", "tc:0", "tb:2", "tc:2", "s0:1", "ta:2", "s0:2", "tb:0", "s1:0", "s2:0",
    "s2:1", "tb:4", "tc:4", "s1:1", "s2:2", "td:0", "s1:2", "ta:4", "s0:3", "s3:0", "prepare",
    "s3:1", "s0:4", "td:2", "s3:2", "s0:5", "s2:3", "s1:3", "s2:4", "s4:0", "s4:1", "s1:4",
    "s1:5", "s4:2", "s3:3", "s2:5", "td:4", "s3:4", "s3:5", "s5:0", "s5:1", "s6:1", "s6:0",
    "s5:2", "peaks:0", "peaks:1", "s4:3", "s6:2", "s4:4", "s7:1", "s7:0", "s4:5", "peaks:2",
    "s7:2", "s5:3", "s5:4", "peaks:3", "s6:3", "s8:0", "peaks:4", "s6:4", "s8:1", "s5:5",
    "peaks:5", "s8:2", "s6:5", "s7:3", "s7:4", "s7:5", "u0", "s8:3", "s9:0", "s8:4", "s9:1",
    "s8:5", "s9:2", "s10:0", "t1:2", "s10:1", "s10:2", "t1:3", "t1:4", "t1:1", "s9:3", "s9:4",
    "s11:0", "s11:1", "u1", "s9:5", "s11:2", "t2:4", "s10:3", "s12:0", "t2:1", "s10:4", "s10:5",
    "pa:4", "s12:1", "t1:0", "s12:2", "s11:3", "t2:3", "t2:2", "t1:5", "s11:4", "both:0",
    "s11:5", "pa:5", "u2", "s12:3", "pb:4", "t2:0", "t2:5", "s12:4", "pb:5", "s12:5", "both:2",
    "pc:4", "pc:5",
)


def kernel(
    tok_h, cot_h, wgt_h, omom_h, codes_h, frm_h, fcm_h, srm_h, scm_h,
    nw_h, nm_h, fs_h, ss_h, frmo_h, fcmo_h, srmo_h, scmo_h, keys_h,
    tok, cot, wgt, omom, codes, frm, fcm, srm, scm, insem,
    nw_o, nm_o, fs_o, ss_o, frm_o, fcm_o, srm_o, scm_o, keys_o, outsem,
    term, xr, cbuf, zf, zs, zr, zc, pf, pcs, pcr, ysf, ysb, yr, zlb, avgt, wbuf, acc,
    wf, rows, rmax, cmx, cmz, fnew, snew, ssem, rsem,
):
    x, zh = lax.axis_index("x"), lax.axis_index("zh")
    y, zl, c = lax.axis_index("y"), lax.axis_index("zl"), lax.axis_index("core")
    here = {"x": x, "zh": zh, "y": y, "zl": zl}

    def at(axis, offset):
        return lax.rem(here[axis] + (4 + offset), 4)

    def to(axis, offset):
        return {axis: at(axis, offset)}

    oc = 1 - c
    partner = {"core": oc}

    barrier = pltpu.get_barrier_semaphore()
    for axis in ("zh", "zl", "y", "x"):
        for o in (2, 1, 3):
            pl.semaphore_signal(barrier, inc=1, device_id=to(axis, o), device_id_type=MESH)
    pl.semaphore_signal(barrier, inc=1, device_id=partner, device_id_type=MESH)

    def token_columns(owner):
        return pl.ds(pl.multiple_of(owner * 512, 512), 512)

    def token_copy(n, owner):
        cols = token_columns(owner)
        return pltpu.make_async_copy(tok_h.at[0, :, cols], tok.at[0, :, cols], insem.at[n])

    owners = (at("x", 2), at("x", 1), at("x", -1), x)
    cot_copy = pltpu.make_async_copy(cot_h, cot, insem.at[4])
    small_copies = [
        pltpu.make_async_copy(src, dst, insem.at[5 + n])
        for n, (src, dst) in enumerate((
            (codes_h, codes), (wgt_h, wgt), (omom_h, omom),
            (frm_h, frm), (fcm_h, fcm), (srm_h, srm), (scm_h, scm),
        ))
    ]
    cot_copy.start()
    for n in range(4):
        token_copy(n, owners[n]).start()
    for copy in small_copies:
        copy.start()

    started, leaving = [], []

    def send(number, src, dst, device):
        copy = pltpu.make_async_remote_copy(
            src_ref=src, dst_ref=dst, send_sem=ssem.at[number], recv_sem=rsem.at[number],
            device_id=device, device_id_type=MESH,
        )
        copy.start()
        started.append(copy)

    def arrived(number, dst):
        pltpu.make_async_remote_copy(
            src_ref=dst, dst_ref=dst, send_sem=ssem.at[number], recv_sem=rsem.at[number],
            device_id=partner, device_id_type=MESH,
        ).wait_recv()

    def leave(src, dst):
        copy = pltpu.make_async_copy(src, dst, outsem.at[len(leaving)])
        copy.start()
        leaving.append(copy)

    def columns(k, n=1):
        return slice(k * T, (k + n) * T)

    def rows_of(start, size):
        return pl.ds(pl.multiple_of(start, size), size)

    def terms(slot, first, count):
        owner = owners[slot]
        part = lax.dot_general(
            tok[0, :, token_columns(owner)], cot[0, :, columns(first, count)],
            (((0,), (0,)), ((), ())), preferred_element_type=f32,
        ).astype(bf16)
        for n in range(count):
            for block in range(4):
                for ab in (0, 1):
                    r = block * T + ab * H
                    term[first + n, slot, ab, block] = part[r:r + H, columns(n)]

    loaded = set()

    def first_terms(slot, k):
        if not loaded:
            cot_copy.wait()
        if slot not in loaded:
            token_copy(slot, owners[slot]).wait()
            loaded.add(slot)
        terms(slot, k, 2)

    def ta(k):
        first_terms(0, k)

    def tb(k):
        first_terms(1, k)

    def tc(k):
        first_terms(2, k)

    def td(k):
        first_terms(3, k)

    def prepare():
        for copy in small_copies:
            copy.wait()
        wf[...] = wgt[...].astype(f32)
        rows[0] = jnp.broadcast_to(frm[...], (T, T)).T
        rows[1] = jnp.broadcast_to(srm[...], (T, T)).T

    def s0(k):
        b = k * PER
        if k == 0:
            pl.semaphore_wait(barrier, 13)
        send(b + XF, term.at[k, 0, 0], xr.at[k, 0, 0], to("x", -1))
        send(b + XF + 1, term.at[k, 0, 1], xr.at[k, 0, 1], to("x", 1))

    def s1(k):
        b = k * PER
        send(b + XD, term.at[k, 1, 0], xr.at[k, 1, 0], to("x", 1))
        send(b + XD + 1, term.at[k, 2, 1], xr.at[k, 1, 1], to("x", -1))

    def s2(k):
        b = k * PER
        for ab, slot, way in ((0, 2, -1), (1, 1, 1)):
            arrived(b + XF + ab, xr.at[k, 0, ab])
            cbuf[k, ab] = (term[k, slot, ab].astype(f32) + xr[k, 0, ab].astype(f32)).astype(bf16)
            send(b + XC + ab, cbuf.at[k, ab], xr.at[k, 2, ab], to("x", way))

    def s3(k):
        b = k * PER
        for ab in (0, 1):
            arrived(b + XD + ab, xr.at[k, 1, ab])
        for ab in (0, 1):
            arrived(b + XC + ab, xr.at[k, 2, ab])

        def total(ab, block):
            value = (
                term[k, 3, ab, block].astype(f32)
                + xr[k, 1, ab, block].astype(f32)
                + xr[k, 2, ab, block].astype(f32)
            )
            zf[k, ab, block] = value
            zs[k, ab, block] = value.astype(bf16)

        far, after, before = at("zh", 2), at("zh", 1), at("zh", -1)
        total(0, far)
        send(b + ZF, zs.at[k, 0, far], zr.at[k, 0, 0], to("zh", -1))
        total(1, far)
        send(b + ZF + 1, zs.at[k, 1, far], zr.at[k, 0, 1], to("zh", 1))
        total(0, after)
        send(b + ZD, zs.at[k, 0, after], zr.at[k, 1, 0], to("zh", 1))
        total(1, before)
        send(b + ZD + 1, zs.at[k, 1, before], zr.at[k, 1, 1], to("zh", -1))
        total(1, after)
        total(0, before)
        total(0, zh)
        total(1, zh)

    def s4(k):
        b = k * PER
        for ab, way in ((0, -1), (1, 1)):
            arrived(b + ZF + ab, zr.at[k, 0, ab])
            zc[k, ab] = (zf[k, ab, at("zh", way)] + zr[k, 0, ab].astype(f32)).astype(bf16)
            send(b + ZC + ab, zc.at[k, ab], zr.at[k, 2, ab], to("zh", way))

    def s5(k):
        b = k * PER
        for ab in (0, 1):
            arrived(b + ZD + ab, zr.at[k, 1, ab])
        for ab in (0, 1):
            arrived(b + ZC + ab, zr.at[k, 2, ab])
        cols = columns(k)
        for ab in (0, 1):
            half = slice(ab * H, (ab + 1) * H)
            gradient = zf[k, ab, zh] + zr[k, 1, ab].astype(f32) + zr[k, 2, ab].astype(f32)
            packed = codes[0, half, cols]
            first_code = (packed >> 4).astype(f32)
            second_code = (packed & 15).astype(f32)
            first_old = jnp.minimum(rows[0, half], fcm[:, cols]) * (first_code - 7.5) / 7.5
            level = (second_code + 1.0) / 16.0
            second_old = jnp.minimum(rows[1, half], scm[:, cols]) * (level * level)
            first_new = beta_one * first_old + (1.0 - beta_one) * gradient
            second_new = beta_two * second_old + (1.0 - beta_two) * gradient * gradient
            update = first_new / bias_one / (jnp.sqrt(second_new / bias_two) + adam_eps)
            pf[k, ab] = inner_rate * (update + weight_decay * wf[half, cols])
            fnew[half, cols] = first_new
            snew[half, cols] = second_new
        pcs[k] = pf[k, oc].astype(bf16)
        send(b + CE, pcs.at[k], pcr.at[k], partner)

    def peaks(k):
        cols = columns(k)
        for m, value in enumerate((jnp.abs(fnew[:, cols]), snew[:, cols])):
            cmx[x, m:m + 1, cols] = jnp.max(value, axis=0, keepdims=True)
            rmax[m] = value if k == 0 else jnp.maximum(rmax[m], value)

    def s6(k):
        b = k * PER
        arrived(b + CE, pcr.at[k])
        both = pf[k, c] + pcr[k].astype(f32)
        ysf[k] = both
        ysb[k] = both.astype(bf16)
        for o in (2, 1, 3):
            theirs = rows_of(at("y", o) * Q, Q)
            send(b + YS + o - 1, ysb.at[k, theirs, :], yr.at[k, o - 1], to("y", o))

    mine = rows_of(y * Q, Q)
    mine_of_block = rows_of(c * H + y * Q, Q)
    my_half = rows_of(c * H, H)
    other_half = rows_of(oc * H, H)

    def s7(k):
        b = k * PER
        for o in (1, 2, 3):
            arrived(b + YS + o - 1, yr.at[k, o - 1])
        zlb[k, zl] = (
            ysf[k, mine, :]
            + yr[k, 0].astype(f32) + yr[k, 1].astype(f32) + yr[k, 2].astype(f32)
        ).astype(bf16)
        for o in (1, 2, 3):
            send(b + LS + o - 1, zlb.at[k, zl], zlb.at[k, zl], to("zl", o))

    def s8(k):
        b = k * PER
        for o in (1, 2, 3):
            arrived(b + LS + o - 1, zlb.at[k, at("zl", -o)])
        parts = [zlb[k, n].astype(f32) for n in range(4)]
        averaged = ((parts[0] + parts[1]) + (parts[2] + parts[3])) / 32.0
        cols = columns(k)
        momentum = outer_beta * omom[mine_of_block, cols] + averaged
        weights = wf[mine_of_block, cols] - outer_rate * (averaged + outer_beta * momentum)
        wbuf[k, x, zh, mine_of_block, :] = weights.astype(bf16)
        for o in (2, 1, 3):
            piece = wbuf.at[k, x, zh, mine_of_block, :]
            send(b + HS + o - 1, piece, piece, to("zh", o))
        avgt[k, mine_of_block, :] = averaged
        for o in (1, 2, 3):
            piece = avgt.at[k, mine_of_block, :]
            send(b + AY + o - 1, piece, piece, to("y", o))

    def s9(k):
        b = k * PER
        for o in (1, 2, 3):
            arrived(b + HS + o - 1, wbuf.at[k, x, at("zh", -o), mine_of_block, :])
        for o in (2, 1, 3):
            piece = wbuf.at[k, x, :, mine_of_block, :]
            send(b + WY + o - 1, piece, piece, to("y", o))

    def half_block(k, at_x, zhs=slice(None)):
        return wbuf.at[k, at_x, zhs, my_half, :]

    def s10(k):
        b = k * PER
        for o in (1, 2, 3):
            theirs = rows_of(c * H + at("y", -o) * Q, Q)
            arrived(b + WY + o - 1, wbuf.at[k, x, :, theirs, :])
        block = half_block(k, x)
        send(b + WX, block, block, to("x", 1))
        send(b + WX + 1, block, block, to("x", -1))
        send(b + WC, block, block, partner)

    def s11(k):
        b = k * PER
        before, after = at("x", -1), at("x", 1)
        arrived(b + WX, half_block(k, before))
        part = half_block(k, before, slice(0, 2))
        send(b + WF, part, part, to("x", 1))
        arrived(b + WX + 1, half_block(k, after))
        part = half_block(k, after, slice(2, 4))
        send(b + WF + 1, part, part, to("x", -1))
        for n, at_x in ((1, before), (2, after)):
            block = half_block(k, at_x)
            send(b + WC + n, block, block, partner)

    def s12(k):
        b = k * PER
        far = at("x", 2)
        arrived(b + WF, half_block(k, far, slice(0, 2)))
        arrived(b + WF + 1, half_block(k, far, slice(2, 4)))
        block = half_block(k, far)
        send(b + WC + 3, block, block, partner)

    def from_partner(k, n, at_x):
        arrived(k * PER + WC + n, wbuf.at[k, at_x, :, other_half, :])

    def block_of(k, at_x):
        return wbuf[k, at_x].reshape(512, T)

    places = (x, at("x", -1), at("x", 1), at("x", 2))

    def product(k, count):
        for n in range(count):
            for i in range(4):
                from_partner(k + n, i, places[i])
        total = None
        for at_x in range(4):
            rhs = jnp.concatenate([block_of(k + n, at_x) for n in range(count)], axis=1)
            part = jnp.dot(tok[0, :, at_x * 512:(at_x + 1) * 512], rhs, preferred_element_type=f32)
            total = part if total is None else total + part
        keys_o[0, :, columns(k, count)] = total.astype(bf16)
        leave(keys_o.at[0, :, columns(k, count)], keys_h.at[0, :, columns(k, count)])

    def both(k):
        product(k, 2)

    def partial(k, i):
        from_partner(k, i, places[i])
        part = jnp.dot(
            tok[0, :, token_columns(places[i])], block_of(k, places[i]),
            preferred_element_type=f32,
        )
        if i > 0:
            part = part + acc[k - NC + 2]
        if i < 3:
            acc[k - NC + 2] = part
        else:
            keys_o[0, :, columns(k)] = part.astype(bf16)
            leave(keys_o.at[0, :, columns(k)], keys_h.at[0, :, columns(k)])

    def pa(k):
        partial(k, 0)

    def pb(k):
        partial(k, 1)
        partial(k, 2)

    def pc(k):
        partial(k, 3)

    def t1(k):
        b = k * PER
        for o in (1, 2, 3):
            theirs = rows_of(c * H + at("y", -o) * Q, Q)
            arrived(b + AY + o - 1, avgt.at[k, theirs, :])
        piece = avgt.at[k, my_half, :]
        send(b + AC, piece, piece, partner)

    def t2(k):
        arrived(k * PER + AC, avgt.at[k, other_half, :])
        cols = columns(k)
        averaged = avgt[k]
        momentum = outer_beta * omom[:, cols] + averaged
        nm_o[:, cols] = momentum
        nw_o[:, cols] = wf[:, cols] - outer_rate * (averaged + outer_beta * momentum)
        if k == NC - 1:
            leave(nm_o, nm_h)
            leave(nw_o, nw_h)

    def u0():
        for o in (1, 2, 3):
            send(CX + o - 1, cmx.at[x], cmx.at[x], to("x", o))

    def u1():
        for o in (1, 2, 3):
            arrived(CX + o - 1, cmx.at[at("x", -o)])
        cmz[zh] = jnp.maximum(jnp.maximum(cmx[0], cmx[1]), jnp.maximum(cmx[2], cmx[3]))
        for o in (1, 2, 3):
            send(CZ + o - 1, cmz.at[zh], cmz.at[zh], to("zh", o))

    def u2():
        for o in (1, 2, 3):
            arrived(CZ + o - 1, cmz.at[at("zh", -o)])
        cols_max = jnp.maximum(jnp.maximum(cmz[0], cmz[1]), jnp.maximum(cmz[2], cmz[3])) + stat_eps
        fcm_o[...] = cols_max[0:1]
        scm_o[...] = cols_max[1:2]
        leave(fcm_o, fcmo_h)
        leave(scm_o, scmo_h)
        for m, (new, rm_o, rm_h, st_o, st_h) in enumerate(
            ((fnew, frm_o, frmo_h, fs_o, fs_h), (snew, srm_o, srmo_h, ss_o, ss_h))
        ):
            flipped = jnp.max(rmax[m].T, axis=0, keepdims=True) + stat_eps
            rm_o[...] = flipped
            leave(rm_o, rm_h)
            rm = jnp.broadcast_to(flipped, (T, T)).T
            for k in range(NC):
                cols = columns(k)
                st_o[0, :, cols] = (
                    new[:, cols] / jnp.minimum(rm, cols_max[m:m + 1, cols])
                ).astype(bf16)
            leave(st_o, st_h)

    stages = {
        f.__name__: f
        for f in (
            ta, tb, tc, td, prepare, s0, s1, s2, s3, s4, s5, peaks, s6, s7, s8, s9, s10, s11, s12,
            both, pa, pb, pc, t1, t2, u0, u1, u2,
        )
    }
    for entry in SCHEDULE:
        name, *chunk = entry.split(":")
        with jax.named_scope("_".join([name, *chunk])):
            stages[name](*map(int, chunk))
    for copy in started:
        copy.wait_send()
    for copy in leaving:
        copy.wait()


def deliver(*refs):
    sources, targets, held, arrive, depart = refs[:9], refs[9:18], refs[18:27], refs[27], refs[28]
    inward = [pltpu.make_async_copy(src, mid, arrive.at[n]) for n, (src, mid) in enumerate(zip(sources, held))]
    outward = [pltpu.make_async_copy(mid, dst, depart.at[n]) for n, (mid, dst) in enumerate(zip(held, targets))]
    for copy in inward:
        copy.start()
    for into, out in zip(inward, outward):
        into.wait()
        out.start()
    for copy in outward:
        copy.wait()


def local(tok, cot, wgt, omom, codes, frm, fcm, srm, scm):
    def out(*shape, dtype=f32):
        return jax.ShapeDtypeStruct(shape, dtype)

    hbm = pl.BlockSpec(memory_space=pl.ANY)
    outs = (
        out(128, 768), out(128, 768),
        out(1, 128, 768, dtype=bf16), out(1, 128, 768, dtype=bf16),
        out(1, 128), out(1, 768), out(1, 128), out(1, 768),
        out(1, 512, 768, dtype=bf16),
    )
    arguments = (tok, cot, wgt, omom, codes, frm, fcm, srm, scm)
    results = pl.pallas_call(
        kernel,
        out_shape=outs,
        in_specs=[hbm] * 9,
        out_specs=(hbm,) * 9,
        scratch_shapes=[
            *(pltpu.VMEM(a.shape, a.dtype) for a in arguments),
            pltpu.SemaphoreType.DMA((12,)),
            *(pltpu.VMEM(a.shape, a.dtype) for a in outs),
            pltpu.SemaphoreType.DMA((16,)),
            pltpu.VMEM((NC, 4, 2, 4, H, T), bf16),
            pltpu.VMEM((NC, 3, 2, 4, H, T), bf16),
            pltpu.VMEM((NC, 2, 4, H, T), bf16),
            pltpu.VMEM((NC, 2, 4, H, T), f32),
            pltpu.VMEM((NC, 2, 4, H, T), bf16),
            pltpu.VMEM((NC, 3, 2, H, T), bf16),
            pltpu.VMEM((NC, 2, H, T), bf16),
            pltpu.VMEM((NC, 2, H, T), f32),
            pltpu.VMEM((NC, H, T), bf16),
            pltpu.VMEM((NC, H, T), bf16),
            pltpu.VMEM((NC, H, T), f32),
            pltpu.VMEM((NC, H, T), bf16),
            pltpu.VMEM((NC, 3, Q, T), bf16),
            pltpu.VMEM((NC, 4, Q, T), bf16),
            pltpu.VMEM((NC, T, T), f32),
            pltpu.VMEM((NC, 4, 4, T, T), bf16),
            pltpu.VMEM((2, 512, T), f32),
            pltpu.VMEM((T, 768), f32),
            pltpu.VMEM((2, T, T), f32),
            pltpu.VMEM((2, T, T), f32),
            pltpu.VMEM((4, 2, 768), f32),
            pltpu.VMEM((4, 2, 768), f32),
            pltpu.VMEM((T, 768), f32),
            pltpu.VMEM((T, 768), f32),
            pltpu.SemaphoreType.DMA((NSEM,)),
            pltpu.SemaphoreType.DMA((NSEM,)),
        ],
        compiler_params=pltpu.CompilerParams(
            collective_id=0, has_side_effects=True, vmem_limit_bytes=67043328
        ),
        name="round",
    )(*arguments)
    return pl.pallas_call(
        deliver,
        out_shape=outs,
        in_specs=[hbm] * 9,
        out_specs=(hbm,) * 9,
        scratch_shapes=[
            *(pltpu.VMEM(a.shape, a.dtype) for a in outs),
            pltpu.SemaphoreType.DMA((9,)),
            pltpu.SemaphoreType.DMA((9,)),
        ],
        compiler_params=pltpu.CompilerParams(vmem_limit_bytes=67043328),
        name="deliver",
    )(*results)


def solution(mesh):
    finer = Mesh(mesh.devices.reshape(4, 4, 2, 4, 4), (*GRP, *FSDP))
    in_specs = (
        P(GRP, FSDP, None), P(GRP, FSDP, None), P(FSDP, None), P(FSDP, None),
        P(GRP, FSDP, None), P(GRP, FSDP), P(GRP, None), P(GRP, FSDP), P(GRP, None),
    )
    out_specs = (
        P(FSDP, None), P(FSDP, None), P(GRP, FSDP, None), P(GRP, FSDP, None),
        P(GRP, FSDP), P(GRP, None), P(GRP, FSDP), P(GRP, None), P(GRP, FSDP, None),
    )
    return jax.shard_map(local, mesh=finer, in_specs=in_specs, out_specs=out_specs, check_vma=False)
```

```python
import jax
import jax.numpy as jnp
from jax import lax
from jax.experimental import pallas as pl
from jax.experimental.pallas import tpu as pltpu
from jax.sharding import Mesh
from jax.sharding import PartitionSpec as P

MESH = pl.DeviceIdType.MESH
GRP = ("zl", "y", "core")
FSDP = ("x", "zh")

beta_one = 0.9
beta_two = 0.95
bias_one = 1.0 - 0.9**10
bias_two = 1.0 - 0.95**10
adam_eps = 1e-08
inner_rate = 0.01
weight_decay = 0.1
outer_rate = 0.7
outer_beta = 0.9
stat_eps = 1e-06

NC = 6
T = 128
H = 64
Q = 16
bf16 = jnp.bfloat16
f32 = jnp.float32

XF, XD, XC, ZF, ZD, ZC = 0, 4, 8, 12, 14, 16
YS, LS, HS, AY, WY = 18, 25, 28, 31, 34
WX, WF, WC, AC = 37, 39, 41, 45
PER = 46
CX, CZ = NC * PER, NC * PER + 3
NSEM = NC * PER + 6

SCHEDULE = (
    "ta:0", "s0:0:0", "ta:4", "s0:4:0", "tc:0", "tb:0", "s1:0:0", "s0:5:0", "tc:4", "ta:2",
    "s2:0:0", "s0:1:0", "tb:4", "s1:4:0", "td:4", "s2:4:0", "s1:5:0", "s0:0:1", "td:0",
    "s3:0:0", "s2:5:0", "s0:5:1", "s2:1:0", "s3:4:0", "prepare", "s0:4:1", "s1:1:0", "s0:2:0",
    "s0:3:0", "s2:0:1", "s3:5:0", "s1:0:1", "s2:5:1", "s1:5:1", "s1:4:1", "s3:1:0", "s0:1:1",
    "tb:2", "s2:4:1", "tc:2", "s2:2:0", "s3:0:1", "s4:0", "s1:2:0", "s0:2:1", "s3:5:1", "s4:5",
    "s2:3:0", "td:2", "s1:3:0", "s3:4:1", "s4:4", "s1:1:1", "s3:2:0", "s0:3:1", "s2:1:1",
    "s2:2:1", "s1:2:1", "s3:3:0", "s1:3:1", "s2:3:1", "s3:1:1", "s4:1", "s5:0", "s3:2:1",
    "s4:2", "s5:5", "s5:4", "s3:3:1", "s7:0", "s4:3", "s7:4", "s5:1", "s7:5", "s8:0", "peaks:0",
    "peaks:1", "s5:2", "s5:3", "peaks:5", "s8:4", "peaks:4", "s7:1", "s8:5", "s7:2", "s7:3",
    "s9:0", "peaks:3", "s8:1", "peaks:2", "u0", "s8:2", "s9:4", "s8:3", "u1", "s10:0", "t1:0",
    "s9:5", "t1:1", "s10:4", "s9:1", "s9:2", "s11:0", "s10:5", "t1:4", "t1:2", "t1:3", "s9:3",
    "s11:4", "t1:5", "t2:2", "s10:1", "s10:2", "t2:3", "pa:4", "t2:1", "pa:0", "s12:4", "s10:3",
    "s11:5", "t2:0", "t2:4", "t2:5", "s11:1", "s12:0", "u2", "s11:2", "pb:4", "s11:3", "pa:2",
    "pb:0", "s12:5", "s12:1", "s12:2", "s12:3", "pb:2", "pc:4", "pc:0", "pc:2",
)


def kernel(
    tok_h, cot_h, wgt_h, omom_h, codes_h, frm_h, fcm_h, srm_h, scm_h,
    nw_h, nm_h, fs_h, ss_h, frmo_h, fcmo_h, srmo_h, scmo_h, keys_h,
    tok, cot, wgt, omom, codes, frm, fcm, srm, scm, insem,
    nw_o, nm_o, fs_o, ss_o, frm_o, fcm_o, srm_o, scm_o, keys_o, outsem,
    term, xr, cbuf, zf, zs, zr, zc, pf, pcs, yr, zlb, avgt, wbuf, acc,
    wf, rows, rmax, cmx, cmz, fnew, snew, ssem, rsem,
):
    x, zh = lax.axis_index("x"), lax.axis_index("zh")
    y, zl, c = lax.axis_index("y"), lax.axis_index("zl"), lax.axis_index("core")
    here = {"x": x, "zh": zh, "y": y, "zl": zl}

    def at(axis, offset):
        return lax.rem(here[axis] + (4 + offset), 4)

    def to(axis, offset):
        return {axis: at(axis, offset)}

    oc = 1 - c
    partner = {"core": oc}

    near = (at("zh", 2), at("zh", 1), at("zh", -1), zh)
    owners = (at("x", 2), at("x", 1), at("x", -1), x)

    def token_columns(owner):
        return pl.ds(pl.multiple_of(owner * 512, 512), 512)

    def token_copies(slot):
        copies = []
        for r in range(4):
            src = pl.ds(pl.multiple_of(owners[slot] * 512 + near[r] * T, T), T)
            dst = pl.ds(pl.multiple_of(owners[slot] * 512 + r * T, T), T)
            copies.append(pltpu.make_async_copy(
                tok_h.at[0, :, src], tok.at[0, :, dst], insem.at[4 * slot + r]
            ))
        return copies

    cot_copy = pltpu.make_async_copy(cot_h, cot, insem.at[16])
    small_copies = [
        pltpu.make_async_copy(src, dst, insem.at[17 + n])
        for n, (src, dst) in enumerate((
            (codes_h, codes), (wgt_h, wgt), (omom_h, omom),
            (frm_h, frm), (fcm_h, fcm), (srm_h, srm), (scm_h, scm),
        ))
    ]
    cot_copy.start()
    for copy in token_copies(0):
        copy.start()

    barrier = pltpu.get_barrier_semaphore()
    far_copy = {"zh": at("zh", 2), "zl": at("zl", 2)}
    partners = [to(axis, o) for axis in ("zh", "zl", "y", "x") for o in (2, 1, 3)]
    partners += [far_copy, partner]
    partners += [{"y": at("y", o), "core": oc} for o in (2, 1, 3)]
    for device in partners:
        pl.semaphore_signal(barrier, inc=1, device_id=device, device_id_type=MESH)

    for slot in (1, 2, 3):
        for copy in token_copies(slot):
            copy.start()
    for copy in small_copies:
        copy.start()

    started, leaving = [], []

    def send(number, src, dst, device):
        copy = pltpu.make_async_remote_copy(
            src_ref=src, dst_ref=dst, send_sem=ssem.at[number], recv_sem=rsem.at[number],
            device_id=device, device_id_type=MESH,
        )
        copy.start()
        started.append(copy)

    def arrived(number, dst):
        pltpu.make_async_remote_copy(
            src_ref=dst, dst_ref=dst, send_sem=ssem.at[number], recv_sem=rsem.at[number],
            device_id=partner, device_id_type=MESH,
        ).wait_recv()

    def leave(src, dst):
        copy = pltpu.make_async_copy(src, dst, outsem.at[len(leaving)])
        copy.start()
        leaving.append(copy)

    def columns(k, n=1):
        return slice(k * T, (k + n) * T)

    def rows_of(start, size):
        return pl.ds(pl.multiple_of(start, size), size)

    def terms(slot, first, count):
        owner = owners[slot]
        part = lax.dot_general(
            tok[0, :, token_columns(owner)], cot[0, :, columns(first, count)],
            (((0,), (0,)), ((), ())), preferred_element_type=f32,
        ).astype(bf16)
        for n in range(count):
            for r in range(4):
                for ab in (0, 1):
                    start = (0, 2, 1, 3)[r] if ab else r
                    start = start * T + ab * H
                    term[first + n, slot, ab, r] = part[start:start + H, columns(n)]

    loaded = set()

    def first_terms(slot, k):
        if not loaded:
            cot_copy.wait()
        if slot not in loaded:
            for copy in token_copies(slot):
                copy.wait()
            loaded.add(slot)
        terms(slot, k, 2)

    def ta(k):
        first_terms(0, k)

    def tb(k):
        first_terms(1, k)

    def tc(k):
        first_terms(2, k)

    def td(k):
        first_terms(3, k)

    def prepare():
        for copy in small_copies:
            copy.wait()
        wf[...] = wgt[...].astype(f32)
        rows[0] = jnp.broadcast_to(frm[...], (T, T)).T
        rows[1] = jnp.broadcast_to(srm[...], (T, T)).T

    def halves(ref, h):
        return ref.at[2 * h:2 * h + 2]

    def s0(k, h):
        b = k * PER + XF + 2 * h
        if k == 0 and h == 0:
            pl.semaphore_wait(barrier, len(partners))
        for ab, way in ((0, -1), (1, 1)):
            send(b + ab, halves(term.at[k, 0, ab], h), halves(xr.at[k, 0, ab], h), to("x", way))

    def s1(k, h):
        b = k * PER + XD + 2 * h
        for ab, slot, way in ((0, 1, 1), (1, 2, -1)):
            send(b + ab, halves(term.at[k, slot, ab], h), halves(xr.at[k, 1, ab], h), to("x", way))

    def s2(k, h):
        b = k * PER + 2 * h
        part = slice(2 * h, 2 * h + 2)
        for ab, slot, way in ((0, 2, -1), (1, 1, 1)):
            arrived(b + XF + ab, halves(xr.at[k, 0, ab], h))
            cbuf[k, ab, part] = (
                term[k, slot, ab, part].astype(f32) + xr[k, 0, ab, part].astype(f32)
            ).astype(bf16)
            send(b + XC + ab, halves(cbuf.at[k, ab], h), halves(xr.at[k, 2, ab], h), to("x", way))

    def s3(k, h):
        b = k * PER + 2 * h
        part = slice(2 * h, 2 * h + 2)
        for ab in (0, 1):
            arrived(b + XD + ab, halves(xr.at[k, 1, ab], h))
        for ab in (0, 1):
            arrived(b + XC + ab, halves(xr.at[k, 2, ab], h))
        for ab in (0, 1):
            value = (
                term[k, 3, ab, part].astype(f32)
                + xr[k, 1, ab, part].astype(f32)
                + xr[k, 2, ab, part].astype(f32)
            )
            if h == 0:
                zs[k, ab] = value.astype(bf16)
            else:
                zf[k, ab] = value
        if h == 0:
            b = k * PER
            send(b + ZF, zs.at[k, 0, 0], zr.at[k, 0, 0], to("zh", -1))
            send(b + ZF + 1, zs.at[k, 1, 0], zr.at[k, 0, 1], to("zh", 1))
            send(b + ZD, zs.at[k, 0, 1], zr.at[k, 1, 0], to("zh", 1))
            send(b + ZD + 1, zs.at[k, 1, 1], zr.at[k, 1, 1], to("zh", -1))

    def s4(k):
        b = k * PER
        for ab, way in ((0, -1), (1, 1)):
            arrived(b + ZF + ab, zr.at[k, 0, ab])
            zc[k, ab] = (zf[k, ab, 0] + zr[k, 0, ab].astype(f32)).astype(bf16)
            send(b + ZC + ab, zc.at[k, ab], zr.at[k, 2, ab], to("zh", way))

    def s5(k):
        b = k * PER
        for ab in (0, 1):
            arrived(b + ZD + ab, zr.at[k, 1, ab])
        for ab in (0, 1):
            arrived(b + ZC + ab, zr.at[k, 2, ab])
        cols = columns(k)
        for ab in (0, 1):
            half = slice(ab * H, (ab + 1) * H)
            gradient = zf[k, ab, 1] + zr[k, 1, ab].astype(f32) + zr[k, 2, ab].astype(f32)
            packed = codes[0, half, cols]
            first_code = (packed >> 4).astype(f32)
            second_code = (packed & 15).astype(f32)
            first_old = jnp.minimum(rows[0, half], fcm[:, cols]) * (first_code - 7.5) / 7.5
            level = (second_code + 1.0) / 16.0
            second_old = jnp.minimum(rows[1, half], scm[:, cols]) * (level * level)
            first_new = beta_one * first_old + (1.0 - beta_one) * gradient
            second_new = beta_two * second_old + (1.0 - beta_two) * gradient * gradient
            update = first_new / bias_one / (jnp.sqrt(second_new / bias_two) + adam_eps)
            pf[k, ab] = inner_rate * (update + weight_decay * wf[half, cols])
            fnew[half, cols] = first_new
            snew[half, cols] = second_new
            pcs[k, ab] = pf[k, ab].astype(bf16)
        for o in (2, 1, 3, 0):
            theirs = rows_of(at("y", o) * Q, Q)
            for other in ((1,) if o == 0 else (0, 1)):
                device = {"y": at("y", o), "core": oc if other else c}
                slot = o + 3 * other - 1 if o else 6
                send(b + YS + slot, pcs.at[k, device["core"], theirs, :], yr.at[k, slot], device)

    def peaks(k):
        cols = columns(k)
        for m, value in enumerate((jnp.abs(fnew[:, cols]), snew[:, cols])):
            cmx[x, m:m + 1, cols] = jnp.max(value, axis=0, keepdims=True)
            rmax[m] = value if k == 0 else jnp.maximum(rmax[m], value)

    mine = rows_of(y * Q, Q)
    mine_of_block = rows_of(c * H + y * Q, Q)
    my_half = rows_of(c * H, H)
    other_half = rows_of(oc * H, H)

    def s7(k):
        b = k * PER
        for slot in range(7):
            arrived(b + YS + slot, yr.at[k, slot])
        total = pf[k, c, mine, :]
        for slot in range(7):
            total = total + yr[k, slot].astype(f32)
        zlb[k, zl] = total.astype(bf16)
        for o in (1, 2, 3):
            send(b + LS + o - 1, zlb.at[k, zl], zlb.at[k, zl], to("zl", o))

    def s8(k):
        b = k * PER
        for o in (1, 2, 3):
            arrived(b + LS + o - 1, zlb.at[k, at("zl", -o)])
        parts = [zlb[k, n].astype(f32) for n in range(4)]
        averaged = ((parts[0] + parts[1]) + (parts[2] + parts[3])) / 32.0
        cols = columns(k)
        momentum = outer_beta * omom[mine_of_block, cols] + averaged
        weights = wf[mine_of_block, cols] - outer_rate * (averaged + outer_beta * momentum)
        wbuf[k, x, zh, mine_of_block, :] = weights.astype(bf16)
        for o in (2, 1, 3):
            piece = wbuf.at[k, x, zh, mine_of_block, :]
            send(b + HS + o - 1, piece, piece, far_copy if o == 2 else to("zh", o))
        avgt[k, mine_of_block, :] = averaged
        for o in (1, 2, 3):
            piece = avgt.at[k, mine_of_block, :]
            send(b + AY + o - 1, piece, piece, to("y", o))

    def s9(k):
        b = k * PER
        for o in (1, 2, 3):
            arrived(b + HS + o - 1, wbuf.at[k, x, at("zh", -o), mine_of_block, :])
        for o in (2, 1, 3):
            piece = wbuf.at[k, x, :, mine_of_block, :]
            send(b + WY + o - 1, piece, piece, to("y", o))

    def half_block(k, at_x, zhs=slice(None)):
        return wbuf.at[k, at_x, zhs, my_half, :]

    def s10(k):
        b = k * PER
        for o in (1, 2, 3):
            theirs = rows_of(c * H + at("y", -o) * Q, Q)
            arrived(b + WY + o - 1, wbuf.at[k, x, :, theirs, :])
        block = half_block(k, x)
        send(b + WX, block, block, to("x", 1))
        send(b + WX + 1, block, block, to("x", -1))
        send(b + WC, block, block, partner)

    def s11(k):
        b = k * PER
        before, after = at("x", -1), at("x", 1)
        arrived(b + WX, half_block(k, before))
        part = half_block(k, before, slice(0, 2))
        send(b + WF, part, part, to("x", 1))
        arrived(b + WX + 1, half_block(k, after))
        part = half_block(k, after, slice(2, 4))
        send(b + WF + 1, part, part, to("x", -1))
        for n, at_x in ((1, before), (2, after)):
            block = half_block(k, at_x)
            send(b + WC + n, block, block, partner)

    def s12(k):
        b = k * PER
        far = at("x", 2)
        arrived(b + WF, half_block(k, far, slice(0, 2)))
        arrived(b + WF + 1, half_block(k, far, slice(2, 4)))
        block = half_block(k, far)
        send(b + WC + 3, block, block, partner)

    def from_partner(k, n, at_x):
        arrived(k * PER + WC + n, wbuf.at[k, at_x, :, other_half, :])

    def block_of(k, at_x):
        return jnp.concatenate([wbuf[k, at_x, block] for block in near], axis=0)

    places = (x, at("x", -1), at("x", 1), at("x", 2))

    def partial(k, i):
        for n in (0, 1):
            from_partner(k + n, i, places[i])
        rhs = jnp.concatenate([block_of(k + n, places[i]) for n in (0, 1)], axis=1)
        part = jnp.dot(tok[0, :, token_columns(places[i])], rhs, preferred_element_type=f32)
        if i > 0:
            part = part + acc[k // 2]
        if i < 3:
            acc[k // 2] = part
        else:
            keys_o[0, :, columns(k, 2)] = part.astype(bf16)
            leave(keys_o.at[0, :, columns(k, 2)], keys_h.at[0, :, columns(k, 2)])

    def pa(k):
        partial(k, 0)

    def pb(k):
        partial(k, 1)
        partial(k, 2)

    def pc(k):
        partial(k, 3)

    def t1(k):
        b = k * PER
        for o in (1, 2, 3):
            theirs = rows_of(c * H + at("y", -o) * Q, Q)
            arrived(b + AY + o - 1, avgt.at[k, theirs, :])
        piece = avgt.at[k, my_half, :]
        send(b + AC, piece, piece, partner)

    def t2(k):
        arrived(k * PER + AC, avgt.at[k, other_half, :])
        cols = columns(k)
        averaged = avgt[k]
        momentum = outer_beta * omom[:, cols] + averaged
        nm_o[:, cols] = momentum
        nw_o[:, cols] = wf[:, cols] - outer_rate * (averaged + outer_beta * momentum)
        if k == NC - 1:
            leave(nm_o, nm_h)
            leave(nw_o, nw_h)

    def u0():
        for o in (1, 2, 3):
            send(CX + o - 1, cmx.at[x], cmx.at[x], to("x", o))

    def u1():
        for o in (1, 2, 3):
            arrived(CX + o - 1, cmx.at[at("x", -o)])
        cmz[zh] = jnp.maximum(jnp.maximum(cmx[0], cmx[1]), jnp.maximum(cmx[2], cmx[3]))
        for o in (1, 2, 3):
            send(CZ + o - 1, cmz.at[zh], cmz.at[zh], to("zh", o))

    def u2():
        for o in (1, 2, 3):
            arrived(CZ + o - 1, cmz.at[at("zh", -o)])
        cols_max = jnp.maximum(jnp.maximum(cmz[0], cmz[1]), jnp.maximum(cmz[2], cmz[3])) + stat_eps
        fcm_o[...] = cols_max[0:1]
        scm_o[...] = cols_max[1:2]
        leave(fcm_o, fcmo_h)
        leave(scm_o, scmo_h)
        for m, (new, rm_o, rm_h, st_o, st_h) in enumerate(
            ((fnew, frm_o, frmo_h, fs_o, fs_h), (snew, srm_o, srmo_h, ss_o, ss_h))
        ):
            flipped = jnp.max(rmax[m].T, axis=0, keepdims=True) + stat_eps
            rm_o[...] = flipped
            leave(rm_o, rm_h)
            rm = jnp.broadcast_to(flipped, (T, T)).T
            for k in range(NC):
                cols = columns(k)
                st_o[0, :, cols] = (
                    new[:, cols] / jnp.minimum(rm, cols_max[m:m + 1, cols])
                ).astype(bf16)
            leave(st_o, st_h)

    stages = {
        f.__name__: f
        for f in (
            ta, tb, tc, td, prepare, s0, s1, s2, s3, s4, s5, peaks, s7, s8, s9, s10, s11, s12,
            pa, pb, pc, t1, t2, u0, u1, u2,
        )
    }
    for entry in SCHEDULE:
        name, *chunk = entry.split(":")
        with jax.named_scope("_".join([name, *chunk])):
            stages[name](*map(int, chunk))
    for copy in started:
        copy.wait_send()
    for copy in leaving:
        copy.wait()


def deliver(*refs):
    sources, targets, held, arrive, depart = refs[:9], refs[9:18], refs[18:27], refs[27], refs[28]
    inward = [pltpu.make_async_copy(src, mid, arrive.at[n]) for n, (src, mid) in enumerate(zip(sources, held))]
    outward = [pltpu.make_async_copy(mid, dst, depart.at[n]) for n, (mid, dst) in enumerate(zip(held, targets))]
    for copy in inward:
        copy.start()
    for into, out in zip(inward, outward):
        into.wait()
        out.start()
    for copy in outward:
        copy.wait()


def local(tok, cot, wgt, omom, codes, frm, fcm, srm, scm):
    def out(*shape, dtype=f32):
        return jax.ShapeDtypeStruct(shape, dtype)

    hbm = pl.BlockSpec(memory_space=pl.ANY)
    outs = (
        out(128, 768), out(128, 768),
        out(1, 128, 768, dtype=bf16), out(1, 128, 768, dtype=bf16),
        out(1, 128), out(1, 768), out(1, 128), out(1, 768),
        out(1, 512, 768, dtype=bf16),
    )
    arguments = (tok, cot, wgt, omom, codes, frm, fcm, srm, scm)
    results = pl.pallas_call(
        kernel,
        out_shape=outs,
        in_specs=[hbm] * 9,
        out_specs=(hbm,) * 9,
        scratch_shapes=[
            *(pltpu.VMEM(a.shape, a.dtype) for a in arguments),
            pltpu.SemaphoreType.DMA((24,)),
            *(pltpu.VMEM(a.shape, a.dtype) for a in outs),
            pltpu.SemaphoreType.DMA((16,)),
            pltpu.VMEM((NC, 4, 2, 4, H, T), bf16),
            pltpu.VMEM((NC, 3, 2, 4, H, T), bf16),
            pltpu.VMEM((NC, 2, 4, H, T), bf16),
            pltpu.VMEM((NC, 2, 2, H, T), f32),
            pltpu.VMEM((NC, 2, 2, H, T), bf16),
            pltpu.VMEM((NC, 3, 2, H, T), bf16),
            pltpu.VMEM((NC, 2, H, T), bf16),
            pltpu.VMEM((NC, 2, H, T), f32),
            pltpu.VMEM((NC, 2, H, T), bf16),
            pltpu.VMEM((NC, 7, Q, T), bf16),
            pltpu.VMEM((NC, 4, Q, T), bf16),
            pltpu.VMEM((NC, T, T), f32),
            pltpu.VMEM((NC, 4, 4, T, T), bf16),
            pltpu.VMEM((NC // 2, 512, 2 * T), f32),
            pltpu.VMEM((T, 768), f32),
            pltpu.VMEM((2, T, T), f32),
            pltpu.VMEM((2, T, T), f32),
            pltpu.VMEM((4, 2, 768), f32),
            pltpu.VMEM((4, 2, 768), f32),
            pltpu.VMEM((T, 768), f32),
            pltpu.VMEM((T, 768), f32),
            pltpu.SemaphoreType.DMA((NSEM,)),
            pltpu.SemaphoreType.DMA((NSEM,)),
        ],
        compiler_params=pltpu.CompilerParams(
            collective_id=0, has_side_effects=True, vmem_limit_bytes=67043328
        ),
        name="round",
    )(*arguments)
    return pl.pallas_call(
        deliver,
        out_shape=outs,
        in_specs=[hbm] * 9,
        out_specs=(hbm,) * 9,
        scratch_shapes=[
            *(pltpu.VMEM(a.shape, a.dtype) for a in outs),
            pltpu.SemaphoreType.DMA((9,)),
            pltpu.SemaphoreType.DMA((9,)),
        ],
        compiler_params=pltpu.CompilerParams(vmem_limit_bytes=67043328),
        name="deliver",
    )(*results)


def solution(mesh):
    finer = Mesh(mesh.devices.reshape(4, 4, 2, 4, 4), (*GRP, *FSDP))
    in_specs = (
        P(GRP, FSDP, None), P(GRP, FSDP, None), P(FSDP, None), P(FSDP, None),
        P(GRP, FSDP, None), P(GRP, FSDP), P(GRP, None), P(GRP, FSDP), P(GRP, None),
    )
    out_specs = (
        P(FSDP, None), P(FSDP, None), P(GRP, FSDP, None), P(GRP, FSDP, None),
        P(GRP, FSDP), P(GRP, None), P(GRP, FSDP), P(GRP, None), P(GRP, FSDP, None),
    )
    return jax.shard_map(local, mesh=finer, in_specs=in_specs, out_specs=out_specs, check_vma=False)
```

```python
import jax
import jax.numpy as jnp
from jax import lax
from jax.experimental import pallas as pl
from jax.experimental.pallas import tpu as pltpu
from jax.sharding import Mesh
from jax.sharding import PartitionSpec as P

MESH = pl.DeviceIdType.MESH
GRP = ("zl", "y", "core")
FSDP = ("x", "zh")

beta_one = 0.9
beta_two = 0.95
bias_one = 1.0 - 0.9**10
bias_two = 1.0 - 0.95**10
adam_eps = 1e-08
inner_rate = 0.01
weight_decay = 0.1
outer_rate = 0.7
outer_beta = 0.9
stat_eps = 1e-06

NC = 6
T = 128
H = 64
Q = 16
bf16 = jnp.bfloat16
f32 = jnp.float32

XF, XD, XC, ZF, ZD, ZC = 0, 4, 8, 12, 14, 16
YS, LS, HS, AY, WY = 18, 25, 28, 31, 34
WX, WF, WC, AC = 37, 41, 43, 47
PER = 48
CX, CZ = NC * PER, NC * PER + 3
NSEM = NC * PER + 6

SCHEDULE = (
    "ta:0", "s0:0:0", "tb:0", "s0:1:0", "tc:0", "s1:0:0", "td:4", "s1:1:0", "ta:4", "s2:0:0",
    "ta:2", "s0:3:0", "s0:2:0", "tc:2", "tb:2", "s2:1:0", "s1:3:0", "td:0", "s0:0:1", "tc:4",
    "s3:0:0", "s2:3:0", "s1:2:0", "s0:1:1", "s2:2:0", "s0:3:1", "td:2", "s1:0:1", "s3:1:0",
    "s2:0:1", "s0:5:0", "s1:1:1", "s3:3:0", "s0:2:1", "s2:1:1", "s0:4:0", "s2:3:1", "s3:2:0",
    "tb:4", "s3:0:1", "s1:3:1", "prepare", "s2:5:0", "s1:5:0", "s4:0", "s0:5:1", "s2:4:0",
    "s3:1:1", "s4:1", "s1:2:1", "s1:4:0", "s3:3:1", "s4:3", "s3:5:0", "s0:4:1", "s2:2:1",
    "s2:5:1", "s3:4:0", "s5:0", "peaks:0", "s1:5:1", "s2:4:1", "s1:4:1", "s5:3", "s3:2:1",
    "s4:2", "s5:1", "peaks:1", "s3:5:1", "s4:5", "s7:0", "s3:4:1", "s4:4", "s7:1", "s7:3",
    "s5:2", "peaks:2", "s8:0", "s5:5", "s8:1", "s5:4", "s8:3", "s7:2", "s7:5", "t1:1",
    "peaks:4", "peaks:5", "t1:0", "peaks:3", "u0", "s9:0", "s7:4", "s8:2", "t1:3", "s9:1",
    "s8:5", "s9:3", "s8:4", "s10:0", "s10:1", "u1", "t1:2", "t1:5", "s9:2", "s10:3", "s9:5",
    "pa:0", "s11:0", "s11:1", "s9:4", "s11:3", "t1:4", "v11:1", "v11:0", "t2:0", "s10:2",
    "s10:5", "s10:4", "pa:2", "v11:3", "pb:0", "s11:2", "s12:1", "s11:5", "v11:2", "s12:0",
    "s12:3", "s11:4", "t2:3", "t2:4", "t2:1", "v11:5", "u2", "t2:2", "t2:5", "pc:0", "v11:4",
    "s12:2", "pb:2", "s12:4", "s12:5", "pa:4", "pb:4", "pc:2", "pc:4",
)


def kernel(
    tok_h, cot_h, wgt_h, omom_h, codes_h, frm_h, fcm_h, srm_h, scm_h,
    nw_h, nm_h, fs_h, ss_h, frmo_h, fcmo_h, srmo_h, scmo_h, keys_h,
    tok, cot, wgt, omom, codes, frm, fcm, srm, scm, insem,
    nw_o, nm_o, fs_o, ss_o, frm_o, fcm_o, srm_o, scm_o, keys_o, outsem,
    term, xr, cbuf, zf, zs, zr, zc, pf, pcs, yr, zlb, avgt, wbuf, acc,
    wf, rows, rmax, cmx, cmz, fnew, snew, ssem, rsem,
):
    x, zh = lax.axis_index("x"), lax.axis_index("zh")
    y, zl, c = lax.axis_index("y"), lax.axis_index("zl"), lax.axis_index("core")
    here = {"x": x, "zh": zh, "y": y, "zl": zl}

    def at(axis, offset):
        return lax.rem(here[axis] + (4 + offset), 4)

    def to(axis, offset):
        return {axis: at(axis, offset)}

    oc = 1 - c
    partner = {"core": oc}

    near = (at("zh", 2), at("zh", 1), at("zh", -1), zh)
    owners = (at("x", 2), at("x", 1), at("x", -1), x)

    def token_columns(owner):
        return pl.ds(pl.multiple_of(owner * 512, 512), 512)

    def token_copies(slot):
        copies = []
        for r in range(4):
            src = pl.ds(pl.multiple_of(owners[slot] * 512 + near[r] * T, T), T)
            dst = pl.ds(pl.multiple_of(owners[slot] * 512 + r * T, T), T)
            copies.append(pltpu.make_async_copy(
                tok_h.at[0, :, src], tok.at[0, :, dst], insem.at[4 * slot + r]
            ))
        return copies

    cot_copy = pltpu.make_async_copy(cot_h, cot, insem.at[16])
    small_copies = [
        pltpu.make_async_copy(src, dst, insem.at[17 + n])
        for n, (src, dst) in enumerate((
            (codes_h, codes), (wgt_h, wgt), (omom_h, omom),
            (frm_h, frm), (fcm_h, fcm), (srm_h, srm), (scm_h, scm),
        ))
    ]
    cot_copy.start()
    for copy in token_copies(0):
        copy.start()

    barrier = pltpu.get_barrier_semaphore()
    far_copy = {"zh": at("zh", 2), "zl": at("zl", 2)}
    partners = [to("zh", 1), to("zh", 3), to("x", 1), to("x", 3)]
    partners += [to(axis, o) for axis in ("zl", "y") for o in (2, 1, 3)]
    partners += [partner]
    partners += [{"y": at("y", o), "core": oc} for o in (2, 1, 3)]
    for device in partners:
        pl.semaphore_signal(barrier, inc=1, device_id=device, device_id_type=MESH)

    for slot in (1, 2, 3):
        for copy in token_copies(slot):
            copy.start()
    for copy in small_copies:
        copy.start()

    started, leaving = [], []

    def send(number, src, dst, device):
        copy = pltpu.make_async_remote_copy(
            src_ref=src, dst_ref=dst, send_sem=ssem.at[number], recv_sem=rsem.at[number],
            device_id=device, device_id_type=MESH,
        )
        copy.start()
        started.append(copy)

    def arrived(number, dst):
        pltpu.make_async_remote_copy(
            src_ref=dst, dst_ref=dst, send_sem=ssem.at[number], recv_sem=rsem.at[number],
            device_id=partner, device_id_type=MESH,
        ).wait_recv()

    def leave(src, dst):
        copy = pltpu.make_async_copy(src, dst, outsem.at[len(leaving)])
        copy.start()
        leaving.append(copy)

    def columns(k, n=1):
        return slice(k * T, (k + n) * T)

    def rows_of(start, size):
        return pl.ds(pl.multiple_of(start, size), size)

    def terms(slot, first, count):
        owner = owners[slot]
        part = lax.dot_general(
            tok[0, :, token_columns(owner)], cot[0, :, columns(first, count)],
            (((0,), (0,)), ((), ())), preferred_element_type=f32,
        ).astype(bf16)
        for n in range(count):
            for r in range(4):
                for ab in (0, 1):
                    start = (0, 2, 1, 3)[r] if ab else r
                    start = start * T + ab * H
                    term[first + n, slot, ab, r] = part[start:start + H, columns(n)]

    loaded = set()

    def first_terms(slot, k):
        if not loaded:
            cot_copy.wait()
        if slot not in loaded:
            for copy in token_copies(slot):
                copy.wait()
            loaded.add(slot)
        terms(slot, k, 2)

    def ta(k):
        first_terms(0, k)

    def tb(k):
        first_terms(1, k)

    def tc(k):
        first_terms(2, k)

    def td(k):
        first_terms(3, k)

    def prepare():
        for copy in small_copies:
            copy.wait()
        wf[...] = wgt[...].astype(f32)
        rows[0] = jnp.broadcast_to(frm[...], (T, T)).T
        rows[1] = jnp.broadcast_to(srm[...], (T, T)).T

    def halves(ref, h):
        return ref.at[2 * h:2 * h + 2]

    def s0(k, h):
        b = k * PER + XF + 2 * h
        if k == 0 and h == 0:
            pl.semaphore_wait(barrier, len(partners))
        for ab, way in ((0, -1), (1, 1)):
            send(b + ab, halves(term.at[k, 0, ab], h), halves(xr.at[k, 0, ab], h), to("x", way))

    def s1(k, h):
        b = k * PER + XD + 2 * h
        for ab, slot, way in ((0, 1, 1), (1, 2, -1)):
            send(b + ab, halves(term.at[k, slot, ab], h), halves(xr.at[k, 1, ab], h), to("x", way))

    def s2(k, h):
        b = k * PER + 2 * h
        part = slice(2 * h, 2 * h + 2)
        for ab, slot, way in ((0, 2, -1), (1, 1, 1)):
            arrived(b + XF + ab, halves(xr.at[k, 0, ab], h))
            cbuf[k, ab, part] = (
                term[k, slot, ab, part].astype(f32) + xr[k, 0, ab, part].astype(f32)
            ).astype(bf16)
            send(b + XC + ab, halves(cbuf.at[k, ab], h), halves(xr.at[k, 2, ab], h), to("x", way))

    def s3(k, h):
        b = k * PER + 2 * h
        part = slice(2 * h, 2 * h + 2)
        for ab in (0, 1):
            arrived(b + XD + ab, halves(xr.at[k, 1, ab], h))
        for ab in (0, 1):
            arrived(b + XC + ab, halves(xr.at[k, 2, ab], h))
        for ab in (0, 1):
            value = (
                term[k, 3, ab, part].astype(f32)
                + xr[k, 1, ab, part].astype(f32)
                + xr[k, 2, ab, part].astype(f32)
            )
            if h == 0:
                zs[k, ab] = value.astype(bf16)
            else:
                zf[k, ab] = value
        if h == 0:
            b = k * PER
            send(b + ZF, zs.at[k, 0, 0], zr.at[k, 0, 0], to("zh", -1))
            send(b + ZF + 1, zs.at[k, 1, 0], zr.at[k, 0, 1], to("zh", 1))
            send(b + ZD, zs.at[k, 0, 1], zr.at[k, 1, 0], to("zh", 1))
            send(b + ZD + 1, zs.at[k, 1, 1], zr.at[k, 1, 1], to("zh", -1))

    def s4(k):
        b = k * PER
        for ab, way in ((0, -1), (1, 1)):
            arrived(b + ZF + ab, zr.at[k, 0, ab])
            zc[k, ab] = (zf[k, ab, 0] + zr[k, 0, ab].astype(f32)).astype(bf16)
            send(b + ZC + ab, zc.at[k, ab], zr.at[k, 2, ab], to("zh", way))

    def s5(k):
        b = k * PER
        for ab in (0, 1):
            arrived(b + ZD + ab, zr.at[k, 1, ab])
        for ab in (0, 1):
            arrived(b + ZC + ab, zr.at[k, 2, ab])
        cols = columns(k)
        for ab in (0, 1):
            half = slice(ab * H, (ab + 1) * H)
            gradient = zf[k, ab, 1] + zr[k, 1, ab].astype(f32) + zr[k, 2, ab].astype(f32)
            packed = codes[0, half, cols]
            first_code = (packed >> 4).astype(f32)
            second_code = (packed & 15).astype(f32)
            first_old = jnp.minimum(rows[0, half], fcm[:, cols]) * (first_code - 7.5) / 7.5
            level = (second_code + 1.0) / 16.0
            second_old = jnp.minimum(rows[1, half], scm[:, cols]) * (level * level)
            first_new = beta_one * first_old + (1.0 - beta_one) * gradient
            second_new = beta_two * second_old + (1.0 - beta_two) * gradient * gradient
            update = first_new / bias_one / (jnp.sqrt(second_new / bias_two) + adam_eps)
            pf[k, ab] = inner_rate * (update + weight_decay * wf[half, cols])
            fnew[half, cols] = first_new
            snew[half, cols] = second_new
            pcs[k, ab] = pf[k, ab].astype(bf16)
        for o in (2, 1, 3, 0):
            theirs = rows_of(at("y", o) * Q, Q)
            for other in ((1,) if o == 0 else (0, 1)):
                device = {"y": at("y", o), "core": oc if other else c}
                slot = o + 3 * other - 1 if o else 6
                send(b + YS + slot, pcs.at[k, device["core"], theirs, :], yr.at[k, slot], device)

    def peaks(k):
        cols = columns(k)
        for m, value in enumerate((jnp.abs(fnew[:, cols]), snew[:, cols])):
            cmx[x, m:m + 1, cols] = jnp.max(value, axis=0, keepdims=True)
            rmax[m] = value if k == 0 else jnp.maximum(rmax[m], value)

    mine = rows_of(y * Q, Q)
    mine_of_block = rows_of(c * H + y * Q, Q)
    my_half = rows_of(c * H, H)
    other_half = rows_of(oc * H, H)

    def s7(k):
        b = k * PER
        for slot in range(7):
            arrived(b + YS + slot, yr.at[k, slot])
        total = pf[k, c, mine, :]
        for slot in range(7):
            total = total + yr[k, slot].astype(f32)
        zlb[k, zl] = total.astype(bf16)
        for o in (1, 2, 3):
            send(b + LS + o - 1, zlb.at[k, zl], zlb.at[k, zl], to("zl", o))

    def s8(k):
        b = k * PER
        for o in (1, 2, 3):
            arrived(b + LS + o - 1, zlb.at[k, at("zl", -o)])
        parts = [zlb[k, n].astype(f32) for n in range(4)]
        averaged = ((parts[0] + parts[1]) + (parts[2] + parts[3])) / 32.0
        cols = columns(k)
        momentum = outer_beta * omom[mine_of_block, cols] + averaged
        weights = wf[mine_of_block, cols] - outer_rate * (averaged + outer_beta * momentum)
        wbuf[k, x, zh, mine_of_block, :] = weights.astype(bf16)
        for o in (2, 1, 3):
            piece = wbuf.at[k, x, zh, mine_of_block, :]
            send(b + HS + o - 1, piece, piece, far_copy if o == 2 else to("zh", o))
        avgt[k, mine_of_block, :] = averaged
        for o in (1, 2, 3):
            piece = avgt.at[k, mine_of_block, :]
            send(b + AY + o - 1, piece, piece, to("y", o))

    def s9(k):
        b = k * PER
        for o in (1, 2, 3):
            arrived(b + HS + o - 1, wbuf.at[k, x, at("zh", -o), mine_of_block, :])
        for o in (2, 1, 3):
            piece = wbuf.at[k, x, :, mine_of_block, :]
            send(b + WY + o - 1, piece, piece, to("y", o))

    def half_block(k, at_x, zhs=slice(None)):
        return wbuf.at[k, at_x, zhs, my_half, :]

    def s10(k):
        b = k * PER
        for o in (1, 2, 3):
            theirs = rows_of(c * H + at("y", -o) * Q, Q)
            arrived(b + WY + o - 1, wbuf.at[k, x, :, theirs, :])
        first, second = half_block(k, x, slice(0, 2)), half_block(k, x, slice(2, 4))
        send(b + WX, first, first, to("x", 1))
        send(b + WX + 1, second, second, to("x", -1))
        send(b + WX + 2, second, second, to("x", 1))
        send(b + WX + 3, first, first, to("x", -1))
        block = half_block(k, x)
        send(b + WC, block, block, partner)

    def s11(k):
        b = k * PER
        part = half_block(k, at("x", -1), slice(0, 2))
        arrived(b + WX, part)
        send(b + WF, part, part, to("x", 1))
        part = half_block(k, at("x", 1), slice(2, 4))
        arrived(b + WX + 1, part)
        send(b + WF + 1, part, part, to("x", -1))

    def v11(k):
        b = k * PER
        before, after = at("x", -1), at("x", 1)
        arrived(b + WX + 2, half_block(k, before, slice(2, 4)))
        arrived(b + WX + 3, half_block(k, after, slice(0, 2)))
        for n, at_x in ((1, before), (2, after)):
            block = half_block(k, at_x)
            send(b + WC + n, block, block, partner)

    def s12(k):
        b = k * PER
        far = at("x", 2)
        arrived(b + WF, half_block(k, far, slice(0, 2)))
        arrived(b + WF + 1, half_block(k, far, slice(2, 4)))
        block = half_block(k, far)
        send(b + WC + 3, block, block, partner)

    def from_partner(k, n, at_x):
        arrived(k * PER + WC + n, wbuf.at[k, at_x, :, other_half, :])

    def block_of(k, at_x):
        return jnp.concatenate([wbuf[k, at_x, block] for block in near], axis=0)

    places = (x, at("x", -1), at("x", 1), at("x", 2))

    def partial(k, i):
        for n in (0, 1):
            from_partner(k + n, i, places[i])
        rhs = jnp.concatenate([block_of(k + n, places[i]) for n in (0, 1)], axis=1)
        part = jnp.dot(tok[0, :, token_columns(places[i])], rhs, preferred_element_type=f32)
        if i > 0:
            part = part + acc[k // 2]
        if i < 3:
            acc[k // 2] = part
        else:
            keys_o[0, :, columns(k, 2)] = part.astype(bf16)
            leave(keys_o.at[0, :, columns(k, 2)], keys_h.at[0, :, columns(k, 2)])

    def pa(k):
        partial(k, 0)

    def pb(k):
        partial(k, 1)
        partial(k, 2)

    def pc(k):
        partial(k, 3)

    def t1(k):
        b = k * PER
        for o in (1, 2, 3):
            theirs = rows_of(c * H + at("y", -o) * Q, Q)
            arrived(b + AY + o - 1, avgt.at[k, theirs, :])
        piece = avgt.at[k, my_half, :]
        send(b + AC, piece, piece, partner)

    def t2(k):
        arrived(k * PER + AC, avgt.at[k, other_half, :])
        cols = columns(k)
        averaged = avgt[k]
        momentum = outer_beta * omom[:, cols] + averaged
        nm_o[:, cols] = momentum
        nw_o[:, cols] = wf[:, cols] - outer_rate * (averaged + outer_beta * momentum)
        if k == NC - 1:
            leave(nm_o, nm_h)
            leave(nw_o, nw_h)

    def u0():
        for o in (1, 2, 3):
            send(CX + o - 1, cmx.at[x], cmx.at[x], to("x", o))

    def u1():
        for o in (1, 2, 3):
            arrived(CX + o - 1, cmx.at[at("x", -o)])
        cmz[zh] = jnp.maximum(jnp.maximum(cmx[0], cmx[1]), jnp.maximum(cmx[2], cmx[3]))
        for o in (1, 2, 3):
            send(CZ + o - 1, cmz.at[zh], cmz.at[zh], to("zh", o))

    def u2():
        for o in (1, 2, 3):
            arrived(CZ + o - 1, cmz.at[at("zh", -o)])
        cols_max = jnp.maximum(jnp.maximum(cmz[0], cmz[1]), jnp.maximum(cmz[2], cmz[3])) + stat_eps
        fcm_o[...] = cols_max[0:1]
        scm_o[...] = cols_max[1:2]
        leave(fcm_o, fcmo_h)
        leave(scm_o, scmo_h)
        for m, (new, rm_o, rm_h, st_o, st_h) in enumerate(
            ((fnew, frm_o, frmo_h, fs_o, fs_h), (snew, srm_o, srmo_h, ss_o, ss_h))
        ):
            flipped = jnp.max(rmax[m].T, axis=0, keepdims=True) + stat_eps
            rm_o[...] = flipped
            leave(rm_o, rm_h)
            rm = jnp.broadcast_to(flipped, (T, T)).T
            for k in range(NC):
                cols = columns(k)
                st_o[0, :, cols] = (
                    new[:, cols] / jnp.minimum(rm, cols_max[m:m + 1, cols])
                ).astype(bf16)
            leave(st_o, st_h)

    stages = {
        f.__name__: f
        for f in (
            ta, tb, tc, td, prepare, s0, s1, s2, s3, s4, s5, peaks, s7, s8, s9, s10, s11, v11, s12,
            pa, pb, pc, t1, t2, u0, u1, u2,
        )
    }
    for entry in SCHEDULE:
        name, *chunk = entry.split(":")
        with jax.named_scope("_".join([name, *chunk])):
            stages[name](*map(int, chunk))
    for copy in started:
        copy.wait_send()
    for copy in leaving:
        copy.wait()


def deliver(*refs):
    sources, targets, held, arrive, depart = refs[:9], refs[9:18], refs[18:27], refs[27], refs[28]
    inward = [pltpu.make_async_copy(src, mid, arrive.at[n]) for n, (src, mid) in enumerate(zip(sources, held))]
    outward = [pltpu.make_async_copy(mid, dst, depart.at[n]) for n, (mid, dst) in enumerate(zip(held, targets))]
    for copy in inward:
        copy.start()
    for into, out in zip(inward, outward):
        into.wait()
        out.start()
    for copy in outward:
        copy.wait()


def local(tok, cot, wgt, omom, codes, frm, fcm, srm, scm):
    def out(*shape, dtype=f32):
        return jax.ShapeDtypeStruct(shape, dtype)

    hbm = pl.BlockSpec(memory_space=pl.ANY)
    outs = (
        out(128, 768), out(128, 768),
        out(1, 128, 768, dtype=bf16), out(1, 128, 768, dtype=bf16),
        out(1, 128), out(1, 768), out(1, 128), out(1, 768),
        out(1, 512, 768, dtype=bf16),
    )
    arguments = (tok, cot, wgt, omom, codes, frm, fcm, srm, scm)
    results = pl.pallas_call(
        kernel,
        out_shape=outs,
        in_specs=[hbm] * 9,
        out_specs=(hbm,) * 9,
        scratch_shapes=[
            *(pltpu.VMEM(a.shape, a.dtype) for a in arguments),
            pltpu.SemaphoreType.DMA((24,)),
            *(pltpu.VMEM(a.shape, a.dtype) for a in outs),
            pltpu.SemaphoreType.DMA((16,)),
            pltpu.VMEM((NC, 4, 2, 4, H, T), bf16),
            pltpu.VMEM((NC, 3, 2, 4, H, T), bf16),
            pltpu.VMEM((NC, 2, 4, H, T), bf16),
            pltpu.VMEM((NC, 2, 2, H, T), f32),
            pltpu.VMEM((NC, 2, 2, H, T), bf16),
            pltpu.VMEM((NC, 3, 2, H, T), bf16),
            pltpu.VMEM((NC, 2, H, T), bf16),
            pltpu.VMEM((NC, 2, H, T), f32),
            pltpu.VMEM((NC, 2, H, T), bf16),
            pltpu.VMEM((NC, 7, Q, T), bf16),
            pltpu.VMEM((NC, 4, Q, T), bf16),
            pltpu.VMEM((NC, T, T), f32),
            pltpu.VMEM((NC, 4, 4, T, T), bf16),
            pltpu.VMEM((NC // 2, 512, 2 * T), f32),
            pltpu.VMEM((T, 768), f32),
            pltpu.VMEM((2, T, T), f32),
            pltpu.VMEM((2, T, T), f32),
            pltpu.VMEM((4, 2, 768), f32),
            pltpu.VMEM((4, 2, 768), f32),
            pltpu.VMEM((T, 768), f32),
            pltpu.VMEM((T, 768), f32),
            pltpu.SemaphoreType.DMA((NSEM,)),
            pltpu.SemaphoreType.DMA((NSEM,)),
        ],
        compiler_params=pltpu.CompilerParams(
            collective_id=0, has_side_effects=True, vmem_limit_bytes=67043328
        ),
        name="round",
    )(*arguments)
    return pl.pallas_call(
        deliver,
        out_shape=outs,
        in_specs=[hbm] * 9,
        out_specs=(hbm,) * 9,
        scratch_shapes=[
            *(pltpu.VMEM(a.shape, a.dtype) for a in outs),
            pltpu.SemaphoreType.DMA((9,)),
            pltpu.SemaphoreType.DMA((9,)),
        ],
        compiler_params=pltpu.CompilerParams(vmem_limit_bytes=67043328),
        name="deliver",
    )(*results)


def solution(mesh):
    finer = Mesh(mesh.devices.reshape(4, 4, 2, 4, 4), (*GRP, *FSDP))
    in_specs = (
        P(GRP, FSDP, None), P(GRP, FSDP, None), P(FSDP, None), P(FSDP, None),
        P(GRP, FSDP, None), P(GRP, FSDP), P(GRP, None), P(GRP, FSDP), P(GRP, None),
    )
    out_specs = (
        P(FSDP, None), P(FSDP, None), P(GRP, FSDP, None), P(GRP, FSDP, None),
        P(GRP, FSDP), P(GRP, None), P(GRP, FSDP), P(GRP, None), P(GRP, FSDP, None),
    )
    return jax.shard_map(local, mesh=finer, in_specs=in_specs, out_specs=out_specs, check_vma=False)
```

```python
import jax
import jax.numpy as jnp
from jax import lax
from jax.experimental import pallas as pl
from jax.experimental.pallas import tpu as pltpu
from jax.sharding import Mesh
from jax.sharding import PartitionSpec as P

MESH = pl.DeviceIdType.MESH
GRP = ("zl", "y", "core")
FSDP = ("x", "zh")

beta_one = 0.9
beta_two = 0.95
bias_one = 1.0 - 0.9**10
bias_two = 1.0 - 0.95**10
adam_eps = 1e-08
inner_rate = 0.01
weight_decay = 0.1
outer_rate = 0.7
outer_beta = 0.9
stat_eps = 1e-06

NC = 6
T = 128
H = 64
Q = 16
bf16 = jnp.bfloat16
f32 = jnp.float32

XF, XD, XC, ZF, ZD, ZC = 0, 4, 8, 12, 14, 16
YS, LS, HS, AY, WY = 18, 25, 28, 31, 34
WX, WF, WC, AC = 37, 41, 43, 47
PER = 48
CX, CZ = NC * PER, NC * PER + 3
GROUPS_OF = (
    0, 0, 1, 1, 2, 2, 3, 3, 2, 2, 3, 3, 4, 4, 5, 5, 5, 5, 6, 6, 6, 6, 6, 6, 6, 7, 7, 7, 8, 8, 8,
    9, 9, 9, 10, 10, 10, 11, 12, 13, 13, 14, 14, 15, 16, 17, 18, 19,
)
PER_SEM = 20
NRECV = NC * PER_SEM + 2
NSEND = 64


def receive_semaphore(number):
    if number >= CX:
        return NC * PER_SEM + (number >= CZ)
    return number // PER * PER_SEM + GROUPS_OF[number % PER]


SCHEDULE = (
    "ta:0", "s0:0:0", "tb:0", "s0:1:0", "tc:0", "s1:0:0", "td:4", "s1:1:0", "ta:4", "s2:0:0",
    "ta:2", "s0:3:0", "s0:2:0", "tc:2", "tb:2", "s2:1:0", "s1:3:0", "td:0", "s0:0:1", "tc:4",
    "s3:0:0", "s2:3:0", "s1:2:0", "s0:1:1", "s2:2:0", "s0:3:1", "td:2", "s1:0:1", "s3:1:0",
    "s2:0:1", "s0:5:0", "s1:1:1", "s3:3:0", "s0:2:1", "s2:1:1", "s0:4:0", "s2:3:1", "s3:2:0",
    "tb:4", "s3:0:1", "s1:3:1", "prepare", "s2:5:0", "s1:5:0", "s4:0", "s0:5:1", "s2:4:0",
    "s3:1:1", "s4:1", "s1:2:1", "s1:4:0", "s3:3:1", "s4:3", "s3:5:0", "s0:4:1", "s2:2:1",
    "s2:5:1", "s3:4:0", "s5:0", "peaks:0", "s1:5:1", "s2:4:1", "s1:4:1", "s5:3", "s3:2:1",
    "s4:2", "s5:1", "peaks:1", "s3:5:1", "s4:5", "s7:0", "s3:4:1", "s4:4", "s7:1", "s7:3",
    "s5:2", "peaks:2", "s8:0", "s5:5", "s8:1", "s5:4", "s8:3", "s7:2", "s7:5", "t1:1",
    "peaks:4", "peaks:5", "t1:0", "peaks:3", "u0", "s9:0", "s7:4", "s8:2", "t1:3", "s9:1",
    "s8:5", "s9:3", "s8:4", "s10:0", "s10:1", "u1", "t1:2", "t1:5", "s9:2", "s10:3", "s9:5",
    "pa:0", "s11:0", "s11:1", "s9:4", "s11:3", "t1:4", "v11:1", "v11:0", "t2:0", "s10:2",
    "s10:5", "s10:4", "pa:2", "v11:3", "pb:0", "s11:2", "s12:1", "s11:5", "v11:2", "s12:0",
    "s12:3", "s11:4", "t2:3", "t2:4", "t2:1", "v11:5", "u2", "t2:2", "t2:5", "pc:0", "v11:4",
    "s12:2", "pb:2", "s12:4", "s12:5", "pa:4", "pb:4", "pc:2", "pc:4",
)


def kernel(
    tok_h, cot_h, wgt_h, omom_h, codes_h, frm_h, fcm_h, srm_h, scm_h,
    nw_h, nm_h, fs_h, ss_h, frmo_h, fcmo_h, srmo_h, scmo_h, keys_h,
    tok, cot, wgt, omom, codes, frm, fcm, srm, scm, insem,
    nw_o, nm_o, fs_o, ss_o, frm_o, fcm_o, srm_o, scm_o, keys_o, outsem,
    term, xr, cbuf, zf, zs, zr, zc, pf, pcs, yr, zlb, avgt, wbuf, acc,
    wf, rows, rmax, cmx, cmz, fnew, snew, ssem, rsem,
):
    x, zh = lax.axis_index("x"), lax.axis_index("zh")
    y, zl, c = lax.axis_index("y"), lax.axis_index("zl"), lax.axis_index("core")
    here = {"x": x, "zh": zh, "y": y, "zl": zl}

    def at(axis, offset):
        return lax.rem(here[axis] + (4 + offset), 4)

    def to(axis, offset):
        return {axis: at(axis, offset)}

    oc = 1 - c
    partner = {"core": oc}

    near = (at("zh", 2), at("zh", 1), at("zh", -1), zh)
    owners = (at("x", 2), at("x", 1), at("x", -1), x)

    def token_columns(owner):
        return pl.ds(pl.multiple_of(owner * 512, 512), 512)

    def token_copies(slot):
        copies = []
        for r in range(4):
            src = pl.ds(pl.multiple_of(owners[slot] * 512 + near[r] * T, T), T)
            dst = pl.ds(pl.multiple_of(owners[slot] * 512 + r * T, T), T)
            copies.append(pltpu.make_async_copy(
                tok_h.at[0, :, src], tok.at[0, :, dst], insem.at[slot]
            ))
        return copies

    cot_copy = pltpu.make_async_copy(cot_h, cot, insem.at[4])
    small_copies = [
        pltpu.make_async_copy(src, dst, insem.at[5 + n])
        for n, (src, dst) in enumerate((
            (codes_h, codes), (wgt_h, wgt), (omom_h, omom),
            (frm_h, frm), (fcm_h, fcm), (srm_h, srm), (scm_h, scm),
        ))
    ]
    cot_copy.start()
    for copy in token_copies(0):
        copy.start()

    barrier = pltpu.get_barrier_semaphore()
    far_copy = {"zh": at("zh", 2), "zl": at("zl", 2)}
    partners = [to("zh", 1), to("zh", 3), to("x", 1), to("x", 3)]
    partners += [to(axis, o) for axis in ("zl", "y") for o in (2, 1, 3)]
    partners += [partner]
    partners += [{"y": at("y", o), "core": oc} for o in (2, 1, 3)]
    for device in partners:
        pl.semaphore_signal(barrier, inc=1, device_id=device, device_id_type=MESH)

    for slot in (1, 2, 3):
        for copy in token_copies(slot):
            copy.start()
    for copy in small_copies:
        copy.start()

    started, leaving = [], []

    def send(number, src, dst, device):
        index = len(started) % NSEND
        if len(started) >= NSEND:
            started[-NSEND].wait_send()
        copy = pltpu.make_async_remote_copy(
            src_ref=src, dst_ref=dst, send_sem=ssem.at[index],
            recv_sem=rsem.at[receive_semaphore(number)],
            device_id=device, device_id_type=MESH,
        )
        copy.start()
        started.append(copy)

    def arrived(number, dst):
        pltpu.make_async_remote_copy(
            src_ref=dst, dst_ref=dst, send_sem=ssem.at[0],
            recv_sem=rsem.at[receive_semaphore(number)], device_id=partner, device_id_type=MESH,
        ).wait_recv()

    def leave(src, dst):
        copy = pltpu.make_async_copy(src, dst, outsem.at[len(leaving)])
        copy.start()
        leaving.append(copy)

    def columns(k, n=1):
        return slice(k * T, (k + n) * T)

    def rows_of(start, size):
        return pl.ds(pl.multiple_of(start, size), size)

    def terms(slot, first, count):
        owner = owners[slot]
        part = lax.dot_general(
            tok[0, :, token_columns(owner)], cot[0, :, columns(first, count)],
            (((0,), (0,)), ((), ())), preferred_element_type=f32,
        ).astype(bf16)
        for n in range(count):
            for r in range(4):
                for ab in (0, 1):
                    start = (0, 2, 1, 3)[r] if ab else r
                    start = start * T + ab * H
                    term[first + n, slot, ab, r] = part[start:start + H, columns(n)]

    loaded = set()

    def first_terms(slot, k):
        if not loaded:
            cot_copy.wait()
        if slot not in loaded:
            cols = token_columns(owners[slot])
            pltpu.make_async_copy(tok_h.at[0, :, cols], tok.at[0, :, cols], insem.at[slot]).wait()
            loaded.add(slot)
        terms(slot, k, 2)

    def ta(k):
        first_terms(0, k)

    def tb(k):
        first_terms(1, k)

    def tc(k):
        first_terms(2, k)

    def td(k):
        first_terms(3, k)

    def prepare():
        for copy in small_copies:
            copy.wait()
        wf[...] = wgt[...].astype(f32)
        rows[0] = jnp.broadcast_to(frm[...], (T, T)).T
        rows[1] = jnp.broadcast_to(srm[...], (T, T)).T

    def halves(ref, h):
        return ref.at[2 * h:2 * h + 2]

    def s0(k, h):
        b = k * PER + XF + 2 * h
        if k == 0 and h == 0:
            pl.semaphore_wait(barrier, len(partners))
        for ab, way in ((0, -1), (1, 1)):
            send(b + ab, halves(term.at[k, 0, ab], h), halves(xr.at[k, 0, ab], h), to("x", way))

    def s1(k, h):
        b = k * PER + XD + 2 * h
        for ab, slot, way in ((0, 1, 1), (1, 2, -1)):
            send(b + ab, halves(term.at[k, slot, ab], h), halves(xr.at[k, 1, ab], h), to("x", way))

    def s2(k, h):
        b = k * PER + 2 * h
        part = slice(2 * h, 2 * h + 2)
        arrived(b + XF, xr.at[k, 0, :, part])
        for ab, slot, way in ((0, 2, -1), (1, 1, 1)):
            cbuf[k, ab, part] = (
                term[k, slot, ab, part].astype(f32) + xr[k, 0, ab, part].astype(f32)
            ).astype(bf16)
            send(b + XC + ab, halves(cbuf.at[k, ab], h), halves(xr.at[k, 2, ab], h), to("x", way))

    def s3(k, h):
        b = k * PER + 2 * h
        part = slice(2 * h, 2 * h + 2)
        arrived(b + XD, xr.at[k, 1:3, :, part])
        for ab in (0, 1):
            value = (
                term[k, 3, ab, part].astype(f32)
                + xr[k, 1, ab, part].astype(f32)
                + xr[k, 2, ab, part].astype(f32)
            )
            if h == 0:
                zs[k, ab] = value.astype(bf16)
            else:
                zf[k, ab] = value
        if h == 0:
            b = k * PER
            send(b + ZF, zs.at[k, 0, 0], zr.at[k, 0, 0], to("zh", -1))
            send(b + ZF + 1, zs.at[k, 1, 0], zr.at[k, 0, 1], to("zh", 1))
            send(b + ZD, zs.at[k, 0, 1], zr.at[k, 1, 0], to("zh", 1))
            send(b + ZD + 1, zs.at[k, 1, 1], zr.at[k, 1, 1], to("zh", -1))

    def s4(k):
        b = k * PER
        arrived(b + ZF, zr.at[k, 0])
        for ab, way in ((0, -1), (1, 1)):
            zc[k, ab] = (zf[k, ab, 0] + zr[k, 0, ab].astype(f32)).astype(bf16)
            send(b + ZC + ab, zc.at[k, ab], zr.at[k, 2, ab], to("zh", way))

    def s5(k):
        b = k * PER
        arrived(b + ZD, zr.at[k, 1:3])
        cols = columns(k)
        for ab in (0, 1):
            half = slice(ab * H, (ab + 1) * H)
            gradient = zf[k, ab, 1] + zr[k, 1, ab].astype(f32) + zr[k, 2, ab].astype(f32)
            packed = codes[0, half, cols]
            first_code = (packed >> 4).astype(f32)
            second_code = (packed & 15).astype(f32)
            first_old = jnp.minimum(rows[0, half], fcm[:, cols]) * (first_code - 7.5) / 7.5
            level = (second_code + 1.0) / 16.0
            second_old = jnp.minimum(rows[1, half], scm[:, cols]) * (level * level)
            first_new = beta_one * first_old + (1.0 - beta_one) * gradient
            second_new = beta_two * second_old + (1.0 - beta_two) * gradient * gradient
            update = first_new / bias_one / (jnp.sqrt(second_new / bias_two) + adam_eps)
            pf[k, ab] = inner_rate * (update + weight_decay * wf[half, cols])
            fnew[half, cols] = first_new
            snew[half, cols] = second_new
            pcs[k, ab] = pf[k, ab].astype(bf16)
        for o in (2, 1, 3, 0):
            theirs = rows_of(at("y", o) * Q, Q)
            for other in ((1,) if o == 0 else (0, 1)):
                device = {"y": at("y", o), "core": oc if other else c}
                slot = o + 3 * other - 1 if o else 6
                send(b + YS + slot, pcs.at[k, device["core"], theirs, :], yr.at[k, slot], device)

    def peaks(k):
        cols = columns(k)
        for m, value in enumerate((jnp.abs(fnew[:, cols]), snew[:, cols])):
            cmx[x, m:m + 1, cols] = jnp.max(value, axis=0, keepdims=True)
            rmax[m] = value if k == 0 else jnp.maximum(rmax[m], value)

    mine = rows_of(y * Q, Q)
    mine_of_block = rows_of(c * H + y * Q, Q)
    my_half = rows_of(c * H, H)
    other_half = rows_of(oc * H, H)

    def s7(k):
        b = k * PER
        arrived(b + YS, yr.at[k])
        total = pf[k, c, mine, :]
        for slot in range(7):
            total = total + yr[k, slot].astype(f32)
        zlb[k, zl] = total.astype(bf16)
        for o in (1, 2, 3):
            send(b + LS + o - 1, zlb.at[k, zl], zlb.at[k, zl], to("zl", o))

    def s8(k):
        b = k * PER
        arrived(b + LS, zlb.at[k, 0:3])
        parts = [zlb[k, n].astype(f32) for n in range(4)]
        averaged = ((parts[0] + parts[1]) + (parts[2] + parts[3])) / 32.0
        cols = columns(k)
        momentum = outer_beta * omom[mine_of_block, cols] + averaged
        weights = wf[mine_of_block, cols] - outer_rate * (averaged + outer_beta * momentum)
        wbuf[k, x, zh, mine_of_block, :] = weights.astype(bf16)
        for o in (2, 1, 3):
            piece = wbuf.at[k, x, zh, mine_of_block, :]
            send(b + HS + o - 1, piece, piece, far_copy if o == 2 else to("zh", o))
        avgt[k, mine_of_block, :] = averaged
        for o in (1, 2, 3):
            piece = avgt.at[k, mine_of_block, :]
            send(b + AY + o - 1, piece, piece, to("y", o))

    def s9(k):
        b = k * PER
        arrived(b + HS, wbuf.at[k, x, 0:3, mine_of_block, :])
        for o in (2, 1, 3):
            piece = wbuf.at[k, x, :, mine_of_block, :]
            send(b + WY + o - 1, piece, piece, to("y", o))

    def half_block(k, at_x, zhs=slice(None)):
        return wbuf.at[k, at_x, zhs, my_half, :]

    def s10(k):
        b = k * PER
        arrived(b + WY, wbuf.at[k, x, 0:3, my_half, :])
        first, second = half_block(k, x, slice(0, 2)), half_block(k, x, slice(2, 4))
        send(b + WX, first, first, to("x", 1))
        send(b + WX + 1, second, second, to("x", -1))
        send(b + WX + 2, second, second, to("x", 1))
        send(b + WX + 3, first, first, to("x", -1))
        block = half_block(k, x)
        send(b + WC, block, block, partner)

    def s11(k):
        b = k * PER
        part = half_block(k, at("x", -1), slice(0, 2))
        arrived(b + WX, part)
        send(b + WF, part, part, to("x", 1))
        part = half_block(k, at("x", 1), slice(2, 4))
        arrived(b + WX + 1, part)
        send(b + WF + 1, part, part, to("x", -1))

    def v11(k):
        b = k * PER
        before, after = at("x", -1), at("x", 1)
        arrived(b + WX + 2, half_block(k, before))
        for n, at_x in ((1, before), (2, after)):
            block = half_block(k, at_x)
            send(b + WC + n, block, block, partner)

    def s12(k):
        b = k * PER
        far = at("x", 2)
        arrived(b + WF, half_block(k, far))
        block = half_block(k, far)
        send(b + WC + 3, block, block, partner)

    def from_partner(k, n, at_x):
        arrived(k * PER + WC + n, wbuf.at[k, at_x, :, other_half, :])

    def block_of(k, at_x):
        return jnp.concatenate([wbuf[k, at_x, block] for block in near], axis=0)

    places = (x, at("x", -1), at("x", 1), at("x", 2))

    def partial(k, i):
        for n in (0, 1):
            from_partner(k + n, i, places[i])
        rhs = jnp.concatenate([block_of(k + n, places[i]) for n in (0, 1)], axis=1)
        part = jnp.dot(tok[0, :, token_columns(places[i])], rhs, preferred_element_type=f32)
        if i > 0:
            part = part + acc[k // 2]
        if i < 3:
            acc[k // 2] = part
        else:
            keys_o[0, :, columns(k, 2)] = part.astype(bf16)
            leave(keys_o.at[0, :, columns(k, 2)], keys_h.at[0, :, columns(k, 2)])

    def pa(k):
        partial(k, 0)

    def pb(k):
        partial(k, 1)
        partial(k, 2)

    def pc(k):
        partial(k, 3)

    def t1(k):
        b = k * PER
        arrived(b + AY, avgt.at[k, 0:3 * Q, :])
        piece = avgt.at[k, my_half, :]
        send(b + AC, piece, piece, partner)

    def t2(k):
        arrived(k * PER + AC, avgt.at[k, other_half, :])
        cols = columns(k)
        averaged = avgt[k]
        momentum = outer_beta * omom[:, cols] + averaged
        nm_o[:, cols] = momentum
        nw_o[:, cols] = wf[:, cols] - outer_rate * (averaged + outer_beta * momentum)
        if k == NC - 1:
            leave(nm_o, nm_h)
            leave(nw_o, nw_h)

    def u0():
        for o in (1, 2, 3):
            send(CX + o - 1, cmx.at[x], cmx.at[x], to("x", o))

    def u1():
        arrived(CX, cmx.at[0:3])
        cmz[zh] = jnp.maximum(jnp.maximum(cmx[0], cmx[1]), jnp.maximum(cmx[2], cmx[3]))
        for o in (1, 2, 3):
            send(CZ + o - 1, cmz.at[zh], cmz.at[zh], to("zh", o))

    def u2():
        arrived(CZ, cmz.at[0:3])
        cols_max = jnp.maximum(jnp.maximum(cmz[0], cmz[1]), jnp.maximum(cmz[2], cmz[3])) + stat_eps
        fcm_o[...] = cols_max[0:1]
        scm_o[...] = cols_max[1:2]
        leave(fcm_o, fcmo_h)
        leave(scm_o, scmo_h)
        for m, (new, rm_o, rm_h, st_o, st_h) in enumerate(
            ((fnew, frm_o, frmo_h, fs_o, fs_h), (snew, srm_o, srmo_h, ss_o, ss_h))
        ):
            flipped = jnp.max(rmax[m].T, axis=0, keepdims=True) + stat_eps
            rm_o[...] = flipped
            leave(rm_o, rm_h)
            rm = jnp.broadcast_to(flipped, (T, T)).T
            for k in range(NC):
                cols = columns(k)
                st_o[0, :, cols] = (
                    new[:, cols] / jnp.minimum(rm, cols_max[m:m + 1, cols])
                ).astype(bf16)
            leave(st_o, st_h)

    stages = {
        f.__name__: f
        for f in (
            ta, tb, tc, td, prepare, s0, s1, s2, s3, s4, s5, peaks, s7, s8, s9, s10, s11, v11, s12,
            pa, pb, pc, t1, t2, u0, u1, u2,
        )
    }
    for entry in SCHEDULE:
        name, *chunk = entry.split(":")
        with jax.named_scope("_".join([name, *chunk])):
            stages[name](*map(int, chunk))
    for copy in started[-NSEND:]:
        copy.wait_send()
    for copy in leaving:
        copy.wait()


def deliver(*refs):
    sources, targets, held, arrive, depart = refs[:9], refs[9:18], refs[18:27], refs[27], refs[28]
    inward = [pltpu.make_async_copy(src, mid, arrive.at[n]) for n, (src, mid) in enumerate(zip(sources, held))]
    outward = [pltpu.make_async_copy(mid, dst, depart.at[n]) for n, (mid, dst) in enumerate(zip(held, targets))]
    for copy in inward:
        copy.start()
    for into, out in zip(inward, outward):
        into.wait()
        out.start()
    for copy in outward:
        copy.wait()


def local(tok, cot, wgt, omom, codes, frm, fcm, srm, scm):
    def out(*shape, dtype=f32):
        return jax.ShapeDtypeStruct(shape, dtype)

    hbm = pl.BlockSpec(memory_space=pl.ANY)
    outs = (
        out(128, 768), out(128, 768),
        out(1, 128, 768, dtype=bf16), out(1, 128, 768, dtype=bf16),
        out(1, 128), out(1, 768), out(1, 128), out(1, 768),
        out(1, 512, 768, dtype=bf16),
    )
    arguments = (tok, cot, wgt, omom, codes, frm, fcm, srm, scm)
    results = pl.pallas_call(
        kernel,
        out_shape=outs,
        in_specs=[hbm] * 9,
        out_specs=(hbm,) * 9,
        scratch_shapes=[
            *(pltpu.VMEM(a.shape, a.dtype) for a in arguments),
            pltpu.SemaphoreType.DMA((12,)),
            *(pltpu.VMEM(a.shape, a.dtype) for a in outs),
            pltpu.SemaphoreType.DMA((11,)),
            pltpu.VMEM((NC, 4, 2, 4, H, T), bf16),
            pltpu.VMEM((NC, 3, 2, 4, H, T), bf16),
            pltpu.VMEM((NC, 2, 4, H, T), bf16),
            pltpu.VMEM((NC, 2, 2, H, T), f32),
            pltpu.VMEM((NC, 2, 2, H, T), bf16),
            pltpu.VMEM((NC, 3, 2, H, T), bf16),
            pltpu.VMEM((NC, 2, H, T), bf16),
            pltpu.VMEM((NC, 2, H, T), f32),
            pltpu.VMEM((NC, 2, H, T), bf16),
            pltpu.VMEM((NC, 7, Q, T), bf16),
            pltpu.VMEM((NC, 4, Q, T), bf16),
            pltpu.VMEM((NC, T, T), f32),
            pltpu.VMEM((NC, 4, 4, T, T), bf16),
            pltpu.VMEM((NC // 2, 512, 2 * T), f32),
            pltpu.VMEM((T, 768), f32),
            pltpu.VMEM((2, T, T), f32),
            pltpu.VMEM((2, T, T), f32),
            pltpu.VMEM((4, 2, 768), f32),
            pltpu.VMEM((4, 2, 768), f32),
            pltpu.VMEM((T, 768), f32),
            pltpu.VMEM((T, 768), f32),
            pltpu.SemaphoreType.DMA((NSEND,)),
            pltpu.SemaphoreType.DMA((NRECV,)),
        ],
        compiler_params=pltpu.CompilerParams(
            collective_id=0, has_side_effects=True, vmem_limit_bytes=67043328
        ),
        name="round",
    )(*arguments)
    return pl.pallas_call(
        deliver,
        out_shape=outs,
        in_specs=[hbm] * 9,
        out_specs=(hbm,) * 9,
        scratch_shapes=[
            *(pltpu.VMEM(a.shape, a.dtype) for a in outs),
            pltpu.SemaphoreType.DMA((9,)),
            pltpu.SemaphoreType.DMA((9,)),
        ],
        compiler_params=pltpu.CompilerParams(vmem_limit_bytes=67043328),
        name="deliver",
    )(*results)


def solution(mesh):
    finer = Mesh(mesh.devices.reshape(4, 4, 2, 4, 4), (*GRP, *FSDP))
    in_specs = (
        P(GRP, FSDP, None), P(GRP, FSDP, None), P(FSDP, None), P(FSDP, None),
        P(GRP, FSDP, None), P(GRP, FSDP), P(GRP, None), P(GRP, FSDP), P(GRP, None),
    )
    out_specs = (
        P(FSDP, None), P(FSDP, None), P(GRP, FSDP, None), P(GRP, FSDP, None),
        P(GRP, FSDP), P(GRP, None), P(GRP, FSDP), P(GRP, None), P(GRP, FSDP, None),
    )
    return jax.shard_map(local, mesh=finer, in_specs=in_specs, out_specs=out_specs, check_vma=False)
```

```python
import jax
import jax.numpy as jnp
from jax import lax
from jax.experimental import pallas as pl
from jax.experimental.pallas import tpu as pltpu
from jax.sharding import Mesh
from jax.sharding import PartitionSpec as P

MESH = pl.DeviceIdType.MESH
GRP = ("zl", "y", "core")
FSDP = ("x", "zh")

beta_one = 0.9
beta_two = 0.95
bias_one = 1.0 - 0.9**10
bias_two = 1.0 - 0.95**10
adam_eps = 1e-08
inner_rate = 0.01
weight_decay = 0.1
outer_rate = 0.7
outer_beta = 0.9
stat_eps = 1e-06

NC = 6
T = 128
H = 64
Q = 16
bf16 = jnp.bfloat16
f32 = jnp.float32

XF, XD, XC, ZF, ZD, ZC = 0, 4, 8, 12, 14, 16
YS, LS, HS, AY, WY = 18, 25, 28, 31, 34
WX, WF, WC, AC = 37, 41, 43, 47
PER = 48
CX, CZ = NC * PER, NC * PER + 3
GROUPS_OF = (
    0, 0, 1, 1, 2, 2, 3, 3, 2, 2, 3, 3, 4, 4, 5, 5, 5, 5, 6, 6, 6, 6, 6, 6, 6, 7, 7, 7, 8, 8, 8,
    9, 9, 9, 10, 10, 10, 11, 12, 13, 13, 14, 14, 15, 16, 17, 18, 19,
)
PER_SEM = 20
NRECV = NC * PER_SEM + 2
NSEND = 32


def receive_semaphore(number):
    if number >= CX:
        return NC * PER_SEM + (number >= CZ)
    return number // PER * PER_SEM + GROUPS_OF[number % PER]


SCHEDULE = (
    "ta:0", "s0:0:0", "tb:0", "s0:1:0", "tc:0", "s1:0:0", "td:4", "s1:1:0", "ta:4", "s2:0:0",
    "ta:2", "s0:3:0", "s0:2:0", "tc:2", "tb:2", "s2:1:0", "s1:3:0", "td:0", "s0:0:1", "tc:4",
    "s3:0:0", "s2:3:0", "s1:2:0", "s0:1:1", "s2:2:0", "s0:3:1", "td:2", "s1:0:1", "s3:1:0",
    "s2:0:1", "s0:5:0", "s1:1:1", "s3:3:0", "s0:2:1", "s2:1:1", "s0:4:0", "s2:3:1", "s3:2:0",
    "tb:4", "s3:0:1", "s1:3:1", "prepare", "s2:5:0", "s1:5:0", "s4:0", "s0:5:1", "s2:4:0",
    "s3:1:1", "s4:1", "s1:2:1", "s1:4:0", "s3:3:1", "s4:3", "s3:5:0", "s0:4:1", "s2:2:1",
    "s2:5:1", "s3:4:0", "s5:0", "peaks:0", "s1:5:1", "s2:4:1", "s1:4:1", "s5:3", "s3:2:1",
    "s4:2", "s5:1", "peaks:1", "s3:5:1", "s4:5", "s7:0", "s3:4:1", "s4:4", "s7:1", "s7:3",
    "s5:2", "peaks:2", "s8:0", "s5:5", "s8:1", "s5:4", "s8:3", "s7:2", "s7:5", "t1:1",
    "peaks:4", "peaks:5", "t1:0", "peaks:3", "u0", "s9:0", "s7:4", "s8:2", "t1:3", "s9:1",
    "s8:5", "s9:3", "s8:4", "s10:0", "s10:1", "u1", "t1:2", "t1:5", "s9:2", "s10:3", "s9:5",
    "pa:0", "s11:0", "s11:1", "s9:4", "s11:3", "t1:4", "v11:1", "v11:0", "t2:0", "s10:2",
    "s10:5", "s10:4", "pa:2", "v11:3", "pb:0", "s11:2", "s12:1", "s11:5", "v11:2", "s12:0",
    "s12:3", "s11:4", "t2:3", "t2:4", "t2:1", "v11:5", "u2", "t2:2", "t2:5", "pc:0", "v11:4",
    "s12:2", "pb:2", "s12:4", "s12:5", "pa:4", "pb:4", "pc:2", "pc:4",
)


def kernel(
    tok_h, cot_h, wgt_h, omom_h, codes_h, frm_h, fcm_h, srm_h, scm_h,
    nw_h, nm_h, fs_h, ss_h, frmo_h, fcmo_h, srmo_h, scmo_h, keys_h,
    tok, cot, wgt, omom, codes, frm, fcm, srm, scm, insem,
    nw_o, nm_o, fs_o, ss_o, frm_o, fcm_o, srm_o, scm_o, keys_o, outsem,
    term, xr, cbuf, zf, zs, zr, zc, pf, pcs, yr, zlb, avgt, wbuf, acc,
    wf, rows, rmax, cmx, cmz, fnew, snew, ssem, rsem,
):
    x, zh = lax.axis_index("x"), lax.axis_index("zh")
    y, zl, c = lax.axis_index("y"), lax.axis_index("zl"), lax.axis_index("core")
    here = {"x": x, "zh": zh, "y": y, "zl": zl}

    def at(axis, offset):
        return lax.rem(here[axis] + (4 + offset), 4)

    def to(axis, offset):
        return {axis: at(axis, offset)}

    oc = 1 - c
    partner = {"core": oc}

    near = (at("zh", 2), at("zh", 1), at("zh", -1), zh)
    owners = (at("x", 2), at("x", 1), at("x", -1), x)

    def token_columns(owner):
        return pl.ds(pl.multiple_of(owner * 512, 512), 512)

    def token_copies(slot):
        copies = []
        for r in range(4):
            src = pl.ds(pl.multiple_of(owners[slot] * 512 + near[r] * T, T), T)
            dst = pl.ds(pl.multiple_of(owners[slot] * 512 + r * T, T), T)
            copies.append(pltpu.make_async_copy(
                tok_h.at[0, :, src], tok.at[0, :, dst], insem.at[slot]
            ))
        return copies

    cot_copy = pltpu.make_async_copy(cot_h, cot, insem.at[4])
    small_copies = [
        pltpu.make_async_copy(src, dst, insem.at[5 + n])
        for n, (src, dst) in enumerate((
            (codes_h, codes), (wgt_h, wgt), (omom_h, omom),
            (frm_h, frm), (fcm_h, fcm), (srm_h, srm), (scm_h, scm),
        ))
    ]
    cot_copy.start()
    for copy in token_copies(0):
        copy.start()

    barrier = pltpu.get_barrier_semaphore()
    far_copy = {"zh": at("zh", 2), "zl": at("zl", 2)}
    partners = [to("zh", 1), to("zh", 3), to("x", 1), to("x", 3)]
    partners += [to(axis, o) for axis in ("zl", "y") for o in (2, 1, 3)]
    partners += [partner]
    partners += [{"y": at("y", o), "core": oc} for o in (2, 1, 3)]
    for device in partners:
        pl.semaphore_signal(barrier, inc=1, device_id=device, device_id_type=MESH)

    for slot in (1, 2, 3):
        for copy in token_copies(slot):
            copy.start()
    for copy in small_copies:
        copy.start()

    started, leaving = [], []

    def send(number, src, dst, device):
        index = len(started) % NSEND
        if len(started) >= NSEND:
            started[-NSEND].wait_send()
        copy = pltpu.make_async_remote_copy(
            src_ref=src, dst_ref=dst, send_sem=ssem.at[index],
            recv_sem=rsem.at[receive_semaphore(number)],
            device_id=device, device_id_type=MESH,
        )
        copy.start()
        started.append(copy)

    def arrived(number, dst):
        pltpu.make_async_remote_copy(
            src_ref=dst, dst_ref=dst, send_sem=ssem.at[0],
            recv_sem=rsem.at[receive_semaphore(number)], device_id=partner, device_id_type=MESH,
        ).wait_recv()

    def leave(src, dst):
        copy = pltpu.make_async_copy(src, dst, outsem.at[len(leaving)])
        copy.start()
        leaving.append(copy)

    def columns(k, n=1):
        return slice(k * T, (k + n) * T)

    def rows_of(start, size):
        return pl.ds(pl.multiple_of(start, size), size)

    def terms(slot, first, count):
        owner = owners[slot]
        part = lax.dot_general(
            tok[0, :, token_columns(owner)], cot[0, :, columns(first, count)],
            (((0,), (0,)), ((), ())), preferred_element_type=f32,
        ).astype(bf16)
        for n in range(count):
            for r in range(4):
                for ab in (0, 1):
                    start = (0, 2, 1, 3)[r] if ab else r
                    start = start * T + ab * H
                    term[first + n, slot, ab, r] = part[start:start + H, columns(n)]

    loaded = set()

    def first_terms(slot, k):
        if not loaded:
            cot_copy.wait()
        if slot not in loaded:
            cols = token_columns(owners[slot])
            pltpu.make_async_copy(tok_h.at[0, :, cols], tok.at[0, :, cols], insem.at[slot]).wait()
            loaded.add(slot)
        terms(slot, k, 2)

    def ta(k):
        first_terms(0, k)

    def tb(k):
        first_terms(1, k)

    def tc(k):
        first_terms(2, k)

    def td(k):
        first_terms(3, k)

    def prepare():
        for copy in small_copies:
            copy.wait()
        wf[...] = wgt[...].astype(f32)
        rows[0] = jnp.broadcast_to(frm[...], (T, T)).T
        rows[1] = jnp.broadcast_to(srm[...], (T, T)).T

    def halves(ref, h):
        return ref.at[2 * h:2 * h + 2]

    def s0(k, h):
        b = k * PER + XF + 2 * h
        if k == 0 and h == 0:
            pl.semaphore_wait(barrier, len(partners))
        for ab, way in ((0, -1), (1, 1)):
            send(b + ab, halves(term.at[k, 0, ab], h), halves(xr.at[k, 0, ab], h), to("x", way))

    def s1(k, h):
        b = k * PER + XD + 2 * h
        for ab, slot, way in ((0, 1, 1), (1, 2, -1)):
            send(b + ab, halves(term.at[k, slot, ab], h), halves(xr.at[k, 1, ab], h), to("x", way))

    def s2(k, h):
        b = k * PER + 2 * h
        part = slice(2 * h, 2 * h + 2)
        arrived(b + XF, xr.at[k, 0, :, part])
        for ab, slot, way in ((0, 2, -1), (1, 1, 1)):
            cbuf[k, ab, part] = (
                term[k, slot, ab, part].astype(f32) + xr[k, 0, ab, part].astype(f32)
            ).astype(bf16)
            send(b + XC + ab, halves(cbuf.at[k, ab], h), halves(xr.at[k, 2, ab], h), to("x", way))

    def s3(k, h):
        b = k * PER + 2 * h
        part = slice(2 * h, 2 * h + 2)
        arrived(b + XD, xr.at[k, 1:3, :, part])
        for ab in (0, 1):
            value = (
                term[k, 3, ab, part].astype(f32)
                + xr[k, 1, ab, part].astype(f32)
                + xr[k, 2, ab, part].astype(f32)
            )
            if h == 0:
                zs[k, ab] = value.astype(bf16)
            else:
                zf[k, ab] = value
        if h == 0:
            b = k * PER
            send(b + ZF, zs.at[k, 0, 0], zr.at[k, 0, 0], to("zh", -1))
            send(b + ZF + 1, zs.at[k, 1, 0], zr.at[k, 0, 1], to("zh", 1))
            send(b + ZD, zs.at[k, 0, 1], zr.at[k, 1, 0], to("zh", 1))
            send(b + ZD + 1, zs.at[k, 1, 1], zr.at[k, 1, 1], to("zh", -1))

    def s4(k):
        b = k * PER
        arrived(b + ZF, zr.at[k, 0])
        for ab, way in ((0, -1), (1, 1)):
            zc[k, ab] = (zf[k, ab, 0] + zr[k, 0, ab].astype(f32)).astype(bf16)
            send(b + ZC + ab, zc.at[k, ab], zr.at[k, 2, ab], to("zh", way))

    def s5(k):
        b = k * PER
        arrived(b + ZD, zr.at[k, 1:3])
        cols = columns(k)
        for ab in (0, 1):
            half = slice(ab * H, (ab + 1) * H)
            gradient = zf[k, ab, 1] + zr[k, 1, ab].astype(f32) + zr[k, 2, ab].astype(f32)
            packed = codes[0, half, cols]
            first_code = (packed >> 4).astype(f32)
            second_code = (packed & 15).astype(f32)
            first_old = jnp.minimum(rows[0, half], fcm[:, cols]) * (first_code - 7.5) / 7.5
            level = (second_code + 1.0) / 16.0
            second_old = jnp.minimum(rows[1, half], scm[:, cols]) * (level * level)
            first_new = beta_one * first_old + (1.0 - beta_one) * gradient
            second_new = beta_two * second_old + (1.0 - beta_two) * gradient * gradient
            update = first_new / bias_one / (jnp.sqrt(second_new / bias_two) + adam_eps)
            pf[k, ab] = inner_rate * (update + weight_decay * wf[half, cols])
            fnew[half, cols] = first_new
            snew[half, cols] = second_new
            pcs[k, ab] = pf[k, ab].astype(bf16)
        for o in (2, 1, 3, 0):
            theirs = rows_of(at("y", o) * Q, Q)
            for other in ((1,) if o == 0 else (0, 1)):
                device = {"y": at("y", o), "core": oc if other else c}
                slot = o + 3 * other - 1 if o else 6
                send(b + YS + slot, pcs.at[k, device["core"], theirs, :], yr.at[k, slot], device)

    def peaks(k):
        cols = columns(k)
        for m, value in enumerate((jnp.abs(fnew[:, cols]), snew[:, cols])):
            cmx[x, m:m + 1, cols] = jnp.max(value, axis=0, keepdims=True)
            rmax[m] = value if k == 0 else jnp.maximum(rmax[m], value)

    mine = rows_of(y * Q, Q)
    mine_of_block = rows_of(c * H + y * Q, Q)
    my_half = rows_of(c * H, H)
    other_half = rows_of(oc * H, H)

    def s7(k):
        b = k * PER
        arrived(b + YS, yr.at[k])
        total = pf[k, c, mine, :]
        for slot in range(7):
            total = total + yr[k, slot].astype(f32)
        zlb[k, zl] = total.astype(bf16)
        for o in (1, 2, 3):
            send(b + LS + o - 1, zlb.at[k, zl], zlb.at[k, zl], to("zl", o))

    def s8(k):
        b = k * PER
        arrived(b + LS, zlb.at[k, 0:3])
        parts = [zlb[k, n].astype(f32) for n in range(4)]
        averaged = ((parts[0] + parts[1]) + (parts[2] + parts[3])) / 32.0
        cols = columns(k)
        momentum = outer_beta * omom[mine_of_block, cols] + averaged
        weights = wf[mine_of_block, cols] - outer_rate * (averaged + outer_beta * momentum)
        wbuf[k, x, zh, mine_of_block, :] = weights.astype(bf16)
        for o in (2, 1, 3):
            piece = wbuf.at[k, x, zh, mine_of_block, :]
            send(b + HS + o - 1, piece, piece, far_copy if o == 2 else to("zh", o))
        avgt[k, mine_of_block, :] = averaged
        for o in (1, 2, 3):
            piece = avgt.at[k, mine_of_block, :]
            send(b + AY + o - 1, piece, piece, to("y", o))

    def s9(k):
        b = k * PER
        arrived(b + HS, wbuf.at[k, x, 0:3, mine_of_block, :])
        for o in (2, 1, 3):
            piece = wbuf.at[k, x, :, mine_of_block, :]
            send(b + WY + o - 1, piece, piece, to("y", o))

    def half_block(k, at_x, zhs=slice(None)):
        return wbuf.at[k, at_x, zhs, my_half, :]

    def s10(k):
        b = k * PER
        arrived(b + WY, wbuf.at[k, x, 0:3, my_half, :])
        first, second = half_block(k, x, slice(0, 2)), half_block(k, x, slice(2, 4))
        send(b + WX, first, first, to("x", 1))
        send(b + WX + 1, second, second, to("x", -1))
        send(b + WX + 2, second, second, to("x", 1))
        send(b + WX + 3, first, first, to("x", -1))
        block = half_block(k, x)
        send(b + WC, block, block, partner)

    def s11(k):
        b = k * PER
        part = half_block(k, at("x", -1), slice(0, 2))
        arrived(b + WX, part)
        send(b + WF, part, part, to("x", 1))
        part = half_block(k, at("x", 1), slice(2, 4))
        arrived(b + WX + 1, part)
        send(b + WF + 1, part, part, to("x", -1))

    def v11(k):
        b = k * PER
        before, after = at("x", -1), at("x", 1)
        arrived(b + WX + 2, half_block(k, before))
        for n, at_x in ((1, before), (2, after)):
            block = half_block(k, at_x)
            send(b + WC + n, block, block, partner)

    def s12(k):
        b = k * PER
        far = at("x", 2)
        arrived(b + WF, half_block(k, far))
        block = half_block(k, far)
        send(b + WC + 3, block, block, partner)

    def from_partner(k, n, at_x):
        arrived(k * PER + WC + n, wbuf.at[k, at_x, :, other_half, :])

    def block_of(k, at_x):
        return jnp.concatenate([wbuf[k, at_x, block] for block in near], axis=0)

    places = (x, at("x", -1), at("x", 1), at("x", 2))

    def partial(k, i):
        for n in (0, 1):
            from_partner(k + n, i, places[i])
        rhs = jnp.concatenate([block_of(k + n, places[i]) for n in (0, 1)], axis=1)
        part = jnp.dot(tok[0, :, token_columns(places[i])], rhs, preferred_element_type=f32)
        if i > 0:
            part = part + acc[k // 2]
        if i < 3:
            acc[k // 2] = part
        else:
            keys_o[0, :, columns(k, 2)] = part.astype(bf16)
            leave(keys_o.at[0, :, columns(k, 2)], keys_h.at[0, :, columns(k, 2)])

    def pa(k):
        partial(k, 0)

    def pb(k):
        partial(k, 1)
        partial(k, 2)

    def pc(k):
        partial(k, 3)

    def t1(k):
        b = k * PER
        arrived(b + AY, avgt.at[k, 0:3 * Q, :])
        piece = avgt.at[k, my_half, :]
        send(b + AC, piece, piece, partner)

    def t2(k):
        arrived(k * PER + AC, avgt.at[k, other_half, :])
        cols = columns(k)
        averaged = avgt[k]
        momentum = outer_beta * omom[:, cols] + averaged
        nm_o[:, cols] = momentum
        nw_o[:, cols] = wf[:, cols] - outer_rate * (averaged + outer_beta * momentum)
        if k == NC - 1:
            leave(nm_o, nm_h)
            leave(nw_o, nw_h)

    def u0():
        for o in (1, 2, 3):
            send(CX + o - 1, cmx.at[x], cmx.at[x], to("x", o))

    def u1():
        arrived(CX, cmx.at[0:3])
        cmz[zh] = jnp.maximum(jnp.maximum(cmx[0], cmx[1]), jnp.maximum(cmx[2], cmx[3]))
        for o in (1, 2, 3):
            send(CZ + o - 1, cmz.at[zh], cmz.at[zh], to("zh", o))

    def u2():
        arrived(CZ, cmz.at[0:3])
        cols_max = jnp.maximum(jnp.maximum(cmz[0], cmz[1]), jnp.maximum(cmz[2], cmz[3])) + stat_eps
        fcm_o[...] = cols_max[0:1]
        scm_o[...] = cols_max[1:2]
        leave(fcm_o, fcmo_h)
        leave(scm_o, scmo_h)
        for m, (new, rm_o, rm_h, st_o, st_h) in enumerate(
            ((fnew, frm_o, frmo_h, fs_o, fs_h), (snew, srm_o, srmo_h, ss_o, ss_h))
        ):
            flipped = jnp.max(rmax[m].T, axis=0, keepdims=True) + stat_eps
            rm_o[...] = flipped
            leave(rm_o, rm_h)
            rm = jnp.broadcast_to(flipped, (T, T)).T
            for k in range(NC):
                cols = columns(k)
                st_o[0, :, cols] = (
                    new[:, cols] / jnp.minimum(rm, cols_max[m:m + 1, cols])
                ).astype(bf16)
            leave(st_o, st_h)

    stages = {
        f.__name__: f
        for f in (
            ta, tb, tc, td, prepare, s0, s1, s2, s3, s4, s5, peaks, s7, s8, s9, s10, s11, v11, s12,
            pa, pb, pc, t1, t2, u0, u1, u2,
        )
    }
    for entry in SCHEDULE:
        name, *chunk = entry.split(":")
        with jax.named_scope("_".join([name, *chunk])):
            stages[name](*map(int, chunk))
    for copy in started[-NSEND:]:
        copy.wait_send()
    for copy in leaving:
        copy.wait()


def deliver(*refs):
    sources, targets, held, arrive, depart = refs[:9], refs[9:18], refs[18:27], refs[27], refs[28]
    moves = []
    for src, mid, dst in zip(sources, held, targets):
        if len(src.shape) == 3 and src.shape[1] > 128:
            for n in range(4):
                part = slice(n * 128, (n + 1) * 128)
                moves.insert(n, (src.at[:, part], mid.at[:, part], dst.at[:, part]))
        else:
            moves.append((src, mid, dst))
    inward = [pltpu.make_async_copy(src, mid, arrive.at[n]) for n, (src, mid, _) in enumerate(moves)]
    outward = [pltpu.make_async_copy(mid, dst, depart.at[n]) for n, (_, mid, dst) in enumerate(moves)]
    for copy in inward:
        copy.start()
    for into, out in zip(inward, outward):
        into.wait()
        out.start()
    for copy in outward:
        copy.wait()


def local(tok, cot, wgt, omom, codes, frm, fcm, srm, scm):
    def out(*shape, dtype=f32):
        return jax.ShapeDtypeStruct(shape, dtype)

    hbm = pl.BlockSpec(memory_space=pl.ANY)
    outs = (
        out(128, 768), out(128, 768),
        out(1, 128, 768, dtype=bf16), out(1, 128, 768, dtype=bf16),
        out(1, 128), out(1, 768), out(1, 128), out(1, 768),
        out(1, 512, 768, dtype=bf16),
    )
    arguments = (tok, cot, wgt, omom, codes, frm, fcm, srm, scm)
    results = pl.pallas_call(
        kernel,
        out_shape=outs,
        in_specs=[hbm] * 9,
        out_specs=(hbm,) * 9,
        scratch_shapes=[
            *(pltpu.VMEM(a.shape, a.dtype) for a in arguments),
            pltpu.SemaphoreType.DMA((12,)),
            *(pltpu.VMEM(a.shape, a.dtype) for a in outs),
            pltpu.SemaphoreType.DMA((11,)),
            pltpu.VMEM((NC, 4, 2, 4, H, T), bf16),
            pltpu.VMEM((NC, 3, 2, 4, H, T), bf16),
            pltpu.VMEM((NC, 2, 4, H, T), bf16),
            pltpu.VMEM((NC, 2, 2, H, T), f32),
            pltpu.VMEM((NC, 2, 2, H, T), bf16),
            pltpu.VMEM((NC, 3, 2, H, T), bf16),
            pltpu.VMEM((NC, 2, H, T), bf16),
            pltpu.VMEM((NC, 2, H, T), f32),
            pltpu.VMEM((NC, 2, H, T), bf16),
            pltpu.VMEM((NC, 7, Q, T), bf16),
            pltpu.VMEM((NC, 4, Q, T), bf16),
            pltpu.VMEM((NC, T, T), f32),
            pltpu.VMEM((NC, 4, 4, T, T), bf16),
            pltpu.VMEM((NC // 2, 512, 2 * T), f32),
            pltpu.VMEM((T, 768), f32),
            pltpu.VMEM((2, T, T), f32),
            pltpu.VMEM((2, T, T), f32),
            pltpu.VMEM((4, 2, 768), f32),
            pltpu.VMEM((4, 2, 768), f32),
            pltpu.VMEM((T, 768), f32),
            pltpu.VMEM((T, 768), f32),
            pltpu.SemaphoreType.DMA((NSEND,)),
            pltpu.SemaphoreType.DMA((NRECV,)),
        ],
        compiler_params=pltpu.CompilerParams(
            collective_id=0, has_side_effects=True, vmem_limit_bytes=67043328
        ),
        name="round",
    )(*arguments)
    return pl.pallas_call(
        deliver,
        out_shape=outs,
        in_specs=[hbm] * 9,
        out_specs=(hbm,) * 9,
        scratch_shapes=[
            *(pltpu.VMEM(a.shape, a.dtype) for a in outs),
            pltpu.SemaphoreType.DMA((12,)),
            pltpu.SemaphoreType.DMA((12,)),
        ],
        compiler_params=pltpu.CompilerParams(vmem_limit_bytes=67043328),
        name="deliver",
    )(*results)


def solution(mesh):
    finer = Mesh(mesh.devices.reshape(4, 4, 2, 4, 4), (*GRP, *FSDP))
    in_specs = (
        P(GRP, FSDP, None), P(GRP, FSDP, None), P(FSDP, None), P(FSDP, None),
        P(GRP, FSDP, None), P(GRP, FSDP), P(GRP, None), P(GRP, FSDP), P(GRP, None),
    )
    out_specs = (
        P(FSDP, None), P(FSDP, None), P(GRP, FSDP, None), P(GRP, FSDP, None),
        P(GRP, FSDP), P(GRP, None), P(GRP, FSDP), P(GRP, None), P(GRP, FSDP, None),
    )
    return jax.shard_map(local, mesh=finer, in_specs=in_specs, out_specs=out_specs, check_vma=False)
```
